128 devices in a mesh: tile: 8 (over x, core), tm: 16 (over z, y).
Axes of the slice: x: 4, y: 4, z: 4, core: 2. Of those that a mesh axis runs over, the one named last changes fastest.
Arguments:
- ocean_heat_anomaly: bfloat16 [512, 192, 1024], P('tm', 'tile'), may hold values from -6 to 6
- observation_reliability: bfloat16 [512, 192, 1024], P('tm', 'tile'), may hold values from 0.099609375 to 1
- swath_date_number: int32 [512], replicated, may hold values from 0 to 511, as said below
- marine_cell_flag: int32 [192, 1024], P('tile'), may hold values 0 or 1
Outputs:
- trend: float32 [512, 192, 1024], P('tm', 'tile')
The draws below stay inside these ranges and needn't reach their ends.
Inputs may be any that keep to these rules, and one draw needn't show every extreme that they name: `swath_date_number`: every day appears exactly once; every index of tm holds the same number of granules of every block of 32 consecutive days, in no particular order.
All inputs are finite; a program needn't handle non-finite values. No bound on the sum of `marine_cell_flag` on one device may be relied on, other than what follows from the above.
Results may differ from the reference program's by a relative error of at most 0.0015.
Values may be sent and summed in bfloat16 or wider, within the bound.
A program may use at most 128 MiB of HBM per device.

```python
import math
import jax
import jax.numpy as jnp
from jax import lax

DAYS_DEV = 32
GRID_WIDTH = 1024
DATE_COUNT = 512
GRID_HEIGHT = 192
N_TM = 16


def draw_swath_date_number(key, part):
    first_key, second_key = jax.random.split(jax.random.fold_in(key, 7))
    share = DAYS_DEV // N_TM
    days_grid = jnp.arange(DATE_COUNT, dtype=jnp.int32).reshape(N_TM, DAYS_DEV)
    block_perm = jax.vmap(lambda sub: jax.random.permutation(sub, DAYS_DEV))(jax.random.split(first_key, N_TM))
    chosen = jnp.take_along_axis(days_grid, block_perm.astype(jnp.int32), axis=1)
    chosen = chosen.reshape(N_TM, N_TM, share).transpose(1, 0, 2).reshape(N_TM, DAYS_DEV)
    source_perm = jax.vmap(lambda sub: jax.random.permutation(sub, DAYS_DEV))(jax.random.split(second_key, N_TM))
    shuffled = jnp.take_along_axis(chosen, source_perm.astype(jnp.int32), axis=1)
    return shuffled.reshape(DATE_COUNT).astype(jnp.int32)


def touch_ends(drawn, stream_key, smallest, largest):
    shape = drawn.shape
    index_at = [jax.random.randint(jax.random.fold_in(stream_key, axis), (), 0, shape[axis]) for axis in range(len(shape))]
    drawn = drawn.at[tuple(index_at)].set(smallest)
    longest = shape.index(max(shape))
    index_at[longest] = (index_at[longest] + 1) % shape[longest]
    return drawn.at[tuple(index_at)].set(largest)


def block_scale(rng, extent, cuts, least, high):
    def one(dim, shards_of):
        steps = jax.random.uniform(jax.random.fold_in(jax.random.fold_in(rng, 6), dim), (shards_of,), jnp.float32, least / len(cuts), high / len(cuts))
        return jnp.repeat(jnp.exp(steps), extent[dim] // shards_of).reshape((-1,) + (1,) * (len(extent) - dim - 1))

    gain = one(*cuts[0])
    for cut in cuts[1:]:
        gain = gain * one(*cut)
    return gain


def normal_values(rng, shape, spread, most, shards=(), held_as=jnp.bfloat16):
    values = jax.random.normal(rng, shape, jnp.float32) * spread
    if len(shards) > 0:
        values = block_scale(rng, shape, shards, -0.22, 0.18) * values
    return jnp.clip(values, min=-most, max=most).astype(held_as)


def setup_inputs(seed: int = 0) -> dict:
    seeds = jax.random.split(jax.random.key(seed), 5)
    ocean_heat_anomaly = normal_values(seeds[0], (DATE_COUNT, GRID_HEIGHT, GRID_WIDTH), 1.0, 6.0, ((0, 16), (1, 8)))
    observation_reliability = jnp.clip(jnp.exp(math.log(1.0) - 2.306499 * jax.random.uniform(seeds[1], (DATE_COUNT, GRID_HEIGHT, GRID_WIDTH), jnp.float32) ** block_scale(seeds[1], (DATE_COUNT, GRID_HEIGHT, GRID_WIDTH), ((0, 16), (1, 8)), -0.2, 0.2)), 0.099609375, 1.0).astype(jnp.bfloat16)
    swath_date_number = draw_swath_date_number(jax.random.fold_in(seeds[4], 71), 0)
    marine_cell_flag = touch_ends((jax.random.randint(seeds[3], (GRID_HEIGHT, GRID_WIDTH), 0, 4) < 3).astype(jnp.int32), jax.random.fold_in(seeds[3], 1), 0, 1)
    return dict(ocean_heat_anomaly=ocean_heat_anomaly, observation_reliability=observation_reliability, swath_date_number=swath_date_number, marine_cell_flag=marine_cell_flag)


DECAY = 0.999
UNIT = 256.0
RIDGE = 0.05


def slope_of(zeroth, first, second, level_sum, slope_sum, ocean):
    det = zeroth * (second + RIDGE) - first * first
    det = jnp.where(ocean > 0, det, jnp.float32(1.0))
    return (first * level_sum - zeroth * slope_sum) / det


def smooth(slopes, ocean):
    padded = jnp.pad(slopes, ((0, 0), (1, 1), (1, 1)))
    rowsum = padded[:, :-2] + padded[:, 1:-1] + padded[:, 2:]
    total = rowsum[:, :, :-2] + rowsum[:, :, 1:-1] + rowsum[:, :, 2:]
    mpad = jnp.pad(ocean, ((1, 1), (1, 1)))
    mrows = mpad[:-2] + mpad[1:-1] + mpad[2:]
    count = mrows[:, :-2] + mrows[:, 1:-1] + mrows[:, 2:]
    return total / jnp.maximum(count, 1.0)[None]


def reference(ocean_heat_anomaly, observation_reliability, swath_date_number, marine_cell_flag):
    ranking_positions = jnp.argsort(swath_date_number).astype(jnp.int32)
    ocean = marine_cell_flag.astype(jnp.float32)
    matrix_items = ocean_heat_anomaly[ranking_positions].astype(jnp.float32)
    weights = observation_reliability[ranking_positions].astype(jnp.float32) * ocean[None]
    step_size = 1.0 / UNIT

    def advance(state, inputs):
        weight_now, value_now = inputs
        zeroth, first, second, level_sum, slope_sum = state
        second = DECAY * (second + 2.0 * step_size * first + step_size * step_size * zeroth)
        first = DECAY * (first + step_size * zeroth)
        zeroth = DECAY * zeroth + weight_now
        slope_sum = DECAY * (slope_sum + step_size * level_sum)
        level_sum = DECAY * level_sum + weight_now * value_now
        slope = slope_of(zeroth, first, second, level_sum, slope_sum, ocean)
        return (zeroth, first, second, level_sum, slope_sum), slope

    empty = jnp.zeros(ocean.shape, jnp.float32)
    start = (empty, empty, empty, empty, empty)
    final_state, slopes = lax.scan(advance, start, (weights, matrix_items))
    return smooth(slopes, ocean)
```

```python
import functools
import math

import jax
import jax.numpy as jnp
from jax import lax
from jax.experimental import pallas as pl
from jax.experimental.pallas import tpu as pltpu
from jax.sharding import PartitionSpec as P

DECAY = 0.999
UNIT = 256.0
RIDGE = 0.05
MESH = pl.DeviceIdType.MESH

OFFSETS = (
    (0, 1), (1, 0), (0, 3), (3, 0), (1, 1), (3, 3), (1, 3), (3, 1),
    (2, 0), (0, 2), (2, 1), (1, 2), (2, 3), (3, 2), (2, 2),
)
CHUNKS = (0, 2, 1)
GROUP = 2


def wait_bytes(ref, sem):
    pltpu.make_async_copy(ref, ref, sem).wait()


def exchange_kernel(
    days, ints_ref, floats_ref, x_ref, w_ref, mask_ref,
    slope_ref, halo_ref, mhalo_ref,
    stage, recv, tsend, trecv, csend, crecv, edge, hrecv, mrecv,
    g_send, g_recv, t_send, t_recv, c_send, c_recv, h_send, h_recv, m_send, m_recv,
):
    me = lax.axis_index("tm")
    tile = lax.axis_index("tile")
    z, y = me // 4, lax.rem(me, 4)
    peers = [lax.rem(z + dz, 4) * 4 + lax.rem(y + dy, 4) for dz, dy in OFFSETS]
    above, below = lax.rem(tile + 7, 8), lax.rem(tile + 1, 8)
    nchunk = len(CHUNKS)

    barrier = pltpu.get_barrier_semaphore()
    for p in peers:
        pl.semaphore_signal(barrier, inc=1, device_id={"tm": p}, device_id_type=MESH)
    for t in (above, below):
        pl.semaphore_signal(barrier, inc=1, device_id={"tile": t}, device_id_type=MESH)

    def place(k, _):
        i = ints_ref[k]
        for c in range(nchunk):
            stage[c, k, 0] = x_ref[i, 4 * c : 4 * c + 4]
            stage[c, k, 1] = w_ref[i, 4 * c : 4 * c + 4]
        return _

    lax.fori_loop(0, days, place, 0)
    for j in range(2):
        i = ints_ref[2 * me + j]
        for c in range(nchunk):
            recv[c, 2 * me + j, 0] = x_ref[i, 4 * c : 4 * c + 4]
            recv[c, 2 * me + j, 1] = w_ref[i, 4 * c : 4 * c + 4]
    pl.semaphore_wait(barrier, len(peers) + 2)

    def remote(src, dst, send, arrive, where):
        pltpu.make_async_remote_copy(
            src_ref=src, dst_ref=dst, send_sem=send, recv_sem=arrive,
            device_id=where, device_id_type=MESH,
        ).start()

    def send_granules(c):
        for p in peers:
            remote(
                stage.at[c, pl.ds(2 * p, 2)], recv.at[c, pl.ds(2 * me, 2)],
                g_send.at[c], g_recv.at[c], {"tm": p},
            )

    def block_totals(c):
        wait_bytes(recv.at[c, pl.ds(0, 30)], g_recv.at[c])
        for g in range(4 // GROUP):
            def add(s, state):
                zeroth, first, second, level, slope = state
                a, u = floats_ref[s], floats_ref[days + s]
                v = recv[c, s, 0, GROUP * g : GROUP * (g + 1)].astype(jnp.float32)
                w = recv[c, s, 1, GROUP * g : GROUP * (g + 1)].astype(jnp.float32) * a
                wu = w * u
                p = w * v
                return (zeroth + w, first + wu, second + wu * u, level + p, slope + p * u)

            empty = jnp.zeros((GROUP, 16, 128), jnp.float32)
            state = lax.fori_loop(0, days, add, (empty,) * 5)
            for m in range(5):
                for q in range(GROUP):
                    for k in range(4):
                        tsend[c, 4 * (GROUP * g + q) + k, m] = state[m][q, 4 * k : 4 * k + 4, :]
        trecv[c, me] = tsend[c, me]
        for p in peers:
            remote(tsend.at[c, p], trecv.at[c, me], t_send.at[c], t_recv.at[c], {"tm": p})

    factor, offset = DECAY**days, days / UNIT

    def carries(c):
        wait_bytes(trecv.at[c, pl.ds(0, 15)], t_recv.at[c])
        state = [jnp.zeros((4, 128), jnp.float32)] * 5
        for b in range(16):
            zeroth, first, second, level, slope = state
            moved = (
                factor * zeroth,
                factor * (first + offset * zeroth),
                factor * (second + (2 * offset) * first + (offset * offset) * zeroth),
                factor * level,
                factor * (slope + offset * level),
            )
            for m in range(5):
                csend[c, b, m] = moved[m]
            state = [moved[m] + trecv[c, b, m] for m in range(5)]
        crecv[c, me] = csend[c, me]
        for p in peers:
            remote(csend.at[c, p], crecv.at[c, me], c_send.at[c], c_recv.at[c], {"tm": p})

    def slopes(c):
        wait_bytes(crecv.at[c, pl.ds(0, 15)], c_recv.at[c])
        for g in range(4 // GROUP):
            start = tuple(
                jnp.stack([
                    jnp.concatenate([crecv[c, 4 * (GROUP * g + q) + k, m] for k in range(4)], axis=0)
                    for q in range(GROUP)
                ])
                for m in range(5)
            )

            def advance(d, state):
                zeroth, first, second, level, slope = state
                s = ints_ref[days + d]
                a, u, ridge = (floats_ref[(2 + n) * days + d] for n in range(3))
                v = recv[c, s, 0, GROUP * g : GROUP * (g + 1)].astype(jnp.float32)
                w = recv[c, s, 1, GROUP * g : GROUP * (g + 1)].astype(jnp.float32) * a
                wu = w * u
                p = w * v
                zeroth, first, second = zeroth + w, first + wu, second + wu * u
                level, slope = level + p, slope + p * u
                det = zeroth * (second + ridge) - first * first
                out = (first * level - zeroth * slope) / det
                for q in range(GROUP):
                    for h in range(2):
                        lanes = pl.ds(128 * (2 * (GROUP * g + q) + h), 128)
                        value = out[q, 8 * h : 8 * h + 8, :]
                        value = jnp.where(mask_ref[8 * c : 8 * c + 8, lanes] > 0, value, 0.0)
                        slope_ref[d, 8 * c : 8 * c + 8, lanes] = value
                        if c == 0:
                            edge[0, d, 2 * (GROUP * g + q) + h : 2 * (GROUP * g + q) + h + 1] = value[0:1]
                        if c == nchunk - 1:
                            edge[1, d, 2 * (GROUP * g + q) + h : 2 * (GROUP * g + q) + h + 1] = value[7:8]
                return (zeroth, first, second, level, slope)

            lax.fori_loop(0, days, advance, start)
        if c == 0:
            remote(edge.at[0], hrecv.at[1], h_send.at[0], h_recv.at[1], {"tile": above})
        if c == nchunk - 1:
            remote(edge.at[1], hrecv.at[0], h_send.at[1], h_recv.at[0], {"tile": below})

    remote(mask_ref.at[0:8], mrecv.at[1], m_send.at[0], m_recv.at[1], {"tile": above})
    remote(mask_ref.at[16:24], mrecv.at[0], m_send.at[1], m_recv.at[0], {"tile": below})

    first, middle, last = CHUNKS
    send_granules(first)
    send_granules(middle)
    block_totals(first)
    send_granules(last)
    block_totals(middle)
    carries(first)
    block_totals(last)
    carries(middle)
    slopes(first)
    carries(last)
    slopes(middle)
    slopes(last)

    for n in range(2):
        wait_bytes(mrecv.at[n], m_recv.at[n])
        wait_bytes(hrecv.at[n], h_recv.at[n])
    halo_ref[...] = hrecv[...]
    mhalo_ref[...] = mrecv[...]
    for c in range(nchunk):
        wait_bytes(stage.at[c, pl.ds(0, 30)], g_send.at[c])
        wait_bytes(tsend.at[c, pl.ds(0, 15)], t_send.at[c])
        wait_bytes(csend.at[c, pl.ds(0, 15)], c_send.at[c])
    for n in range(2):
        wait_bytes(edge.at[n], h_send.at[n])
        wait_bytes(mask_ref.at[0:8], m_send.at[n])


def box_sum(field, up, down):
    column = lax.broadcasted_iota(jnp.int32, field.shape, 1)
    rows = (
        field
        + jnp.concatenate([up, field[:-1]], axis=0)
        + jnp.concatenate([field[1:], down], axis=0)
    )
    width = field.shape[1]
    left = jnp.where(column == 0, 0.0, pltpu.roll(rows, 1, 1))
    right = jnp.where(column == width - 1, 0.0, pltpu.roll(rows, width - 1, 1))
    return rows + left + right


def row_of(pieces):
    return jnp.concatenate([pieces[k : k + 1] for k in range(pieces.shape[0])], axis=1)


def smooth_kernel(valid_ref, slope_ref, halo_ref, mask_ref, mhalo_ref, out_ref, inverse):
    step, per = pl.program_id(0), slope_ref.shape[0]
    has_up, has_down = valid_ref[0], valid_ref[1]

    @pl.when(step == 0)
    def _():
        count = box_sum(
            mask_ref[...].astype(jnp.float32),
            mhalo_ref[0, 7:8].astype(jnp.float32) * has_up,
            mhalo_ref[1, 0:1].astype(jnp.float32) * has_down,
        )
        inverse[...] = 1.0 / jnp.maximum(count, 1.0)

    for n in range(per):
        d = step * per + n
        up = row_of(halo_ref[0, d]) * has_up
        down = row_of(halo_ref[1, d]) * has_down
        out_ref[n] = box_sum(slope_ref[n], up, down) * inverse[...]


def tables(swath_date_number, me, n, days):
    index = jnp.arange(days, dtype=jnp.int32)
    all_days = swath_date_number.reshape(n, days)
    block = all_days // days
    mine = lax.dynamic_index_in_dim(block, me, 0, keepdims=False)
    key = mine * days + index
    rank = jnp.sum((key[None, :] < key[:, None]).astype(jnp.int32), axis=1)
    order = jnp.sum(jnp.where(rank[None, :] == index[:, None], index[None, :], 0), axis=1)
    inside = block == me
    before = (index[None, :] < index[:, None])[None] & inside[:, None, :]
    place = jnp.sum(before.astype(jnp.int32), axis=2)
    slot = 2 * jnp.arange(n, dtype=jnp.int32)[:, None] + place
    hit = (all_days - me * days)[None] == index[:, None, None]
    slot_of_day = jnp.sum(jnp.where(hit, slot[None], 0), axis=(1, 2))
    day_of_slot = jnp.sum(jnp.where(slot_of_day[None, :] == index[:, None], index[None, :], 0), axis=1)
    ints = jnp.concatenate([order, slot_of_day])
    lag_slot = (days - 1 - day_of_slot).astype(jnp.float32)
    lag_day = (days - 1 - index).astype(jnp.float32)
    decay_slot = jnp.exp(lag_slot * math.log(DECAY))
    decay_day = jnp.exp(lag_day * math.log(DECAY))
    floats = jnp.concatenate(
        [decay_slot, lag_slot / UNIT, decay_day, lag_day / UNIT, RIDGE * decay_day]
    )
    return ints, floats


def tiled(array):
    days, rows, width = array.shape
    parts = array.reshape(days, rows // 8, 8, width // 256, 2, 128)
    return parts.transpose(0, 1, 3, 4, 2, 5).reshape(days, rows // 8 * (width // 256), 16, 128)


def on_device(ocean_heat_anomaly, observation_reliability, swath_date_number, marine_cell_flag):
    n, me, tile = lax.axis_size("tm"), lax.axis_index("tm"), lax.axis_index("tile")
    days, rows, width = ocean_heat_anomaly.shape
    ints, floats = tables(swath_date_number, me, n, days)
    f32, bf16 = jnp.float32, jnp.bfloat16
    smem = pl.BlockSpec(memory_space=pltpu.SMEM)
    vmem = pl.BlockSpec(memory_space=pltpu.VMEM)
    sem = pltpu.SemaphoreType.DMA
    slope, halo, mhalo = pl.pallas_call(
        functools.partial(exchange_kernel, days),
        out_shape=(
            jax.ShapeDtypeStruct((days, rows, width), f32),
            jax.ShapeDtypeStruct((2, days, width // 128, 128), f32),
            jax.ShapeDtypeStruct((2, 8, width), jnp.int32),
        ),
        in_specs=[smem, smem, vmem, vmem, vmem],
        out_specs=(vmem, vmem, vmem),
        scratch_shapes=[
            pltpu.VMEM((3, days, 2, 4, 16, 128), bf16),
            pltpu.VMEM((3, days, 2, 4, 16, 128), bf16),
            pltpu.VMEM((3, n, 5, 4, 128), f32),
            pltpu.VMEM((3, n, 5, 4, 128), f32),
            pltpu.VMEM((3, n, 5, 4, 128), f32),
            pltpu.VMEM((3, n, 5, 4, 128), f32),
            pltpu.VMEM((2, days, width // 128, 128), f32),
            pltpu.VMEM((2, days, width // 128, 128), f32),
            pltpu.VMEM((2, 8, width), jnp.int32),
        ] + [sem((3,))] * 6 + [sem((2,))] * 4,
        compiler_params=pltpu.CompilerParams(collective_id=0, has_side_effects=True),
    )(ints, floats, tiled(ocean_heat_anomaly), tiled(observation_reliability), marine_cell_flag)
    valid = jnp.stack([tile > 0, tile < lax.axis_size("tile") - 1]).astype(f32)
    per = 4
    whole = lambda *shape: pl.BlockSpec(shape, lambda i: (0,) * len(shape))
    return pl.pallas_call(
        smooth_kernel,
        grid=(days // per,),
        out_shape=jax.ShapeDtypeStruct((days, rows, width), f32),
        in_specs=[
            smem,
            pl.BlockSpec((per, rows, width), lambda i: (i, 0, 0)),
            whole(2, days, width // 128, 128),
            whole(rows, width),
            whole(2, 8, width),
        ],
        out_specs=pl.BlockSpec((per, rows, width), lambda i: (i, 0, 0)),
        scratch_shapes=[pltpu.VMEM((rows, width), f32)],
    )(valid, slope, halo, marine_cell_flag, mhalo)


def solution(mesh):
    in_specs = (P("tm", "tile", None), P("tm", "tile", None), P(), P("tile", None))
    out_specs = P("tm", "tile", None)
    return jax.shard_map(
        on_device, mesh=mesh, in_specs=in_specs, out_specs=out_specs, check_vma=False
    )
```

```python
import functools
import math

import jax
import jax.numpy as jnp
from jax import lax
from jax.experimental import pallas as pl
from jax.experimental.pallas import tpu as pltpu
from jax.sharding import PartitionSpec as P

DECAY = 0.999
UNIT = 256.0
RIDGE = 0.05
MESH = pl.DeviceIdType.MESH

OFFSETS = (
    (0, 1), (1, 0), (0, 3), (3, 0), (1, 1), (3, 3), (1, 3), (3, 1),
    (2, 0), (0, 2), (2, 1), (1, 2), (2, 3), (3, 2), (2, 2),
)
CHUNKS = (0, 2, 1)
GROUP = 2


def wait_bytes(ref, sem):
    pltpu.make_async_copy(ref, ref, sem).wait()


def write_tables(days, me, swath_ref, ints_vec, floats_vec):
    swath = swath_ref[...]
    row, lane = (lax.broadcasted_iota(jnp.int32, swath.shape, k) for k in range(2))
    per = 128 // days
    block, group, index = swath // days, lane // days, lax.rem(lane, days)
    source = per * row + group

    owned = jnp.sum(jnp.where(source == me, block, 0), axis=0, keepdims=True)
    number, lane16 = (lax.broadcasted_iota(jnp.int32, (16, 128), k) for k in range(2))
    index16 = lax.rem(lane16, days)
    match = (number == owned) & (lane16 // days == lax.rem(me, per))
    early = jnp.min(jnp.where(match, index16, days - 1), axis=1, keepdims=True)
    late = jnp.max(jnp.where(match, index16, 0), axis=1, keepdims=True)
    diagonal = number == lane16
    ints_vec[0:1] = jnp.sum(jnp.where(diagonal, early, 0), axis=0, keepdims=True)
    ints_vec[1:2] = jnp.sum(jnp.where(diagonal, late, 0), axis=0, keepdims=True)

    second = jnp.zeros(swath.shape, jnp.int32)
    for g in range(per):
        inside = (block == me) & (group == g)
        latest = jnp.max(jnp.where(inside, index, -1), axis=1, keepdims=True)
        second = jnp.where(inside & (index == latest), 1, second)
    slot = 2 * source + second
    day, lane32 = (lax.broadcasted_iota(jnp.int32, (days, 128), k) for k in range(2))
    hit = jnp.zeros((days, 128), jnp.int32)
    for r in range(swath.shape[0]):
        hit += jnp.where(swath[r : r + 1] == days * me + day, slot[r : r + 1], 0)
    arrived = jnp.clip(jnp.sum(hit, axis=1, keepdims=True), 0, days - 1)
    ints_vec[2:3] = jnp.sum(jnp.where(day == lane32, arrived, 0), axis=0, keepdims=True)

    lag = (days - 1 - lax.broadcasted_iota(jnp.int32, (1, 128), 1)).astype(jnp.float32)
    decay = jnp.exp(lag * math.log(DECAY))
    floats_vec[0:1] = decay
    floats_vec[1:2] = lag * (1.0 / UNIT)
    floats_vec[2:3] = RIDGE * decay


def exchange_kernel(
    days, swath_ref, x_hbm, w_hbm, mask_hbm,
    slope_ref, halo_ref, mhalo_ref,
    x_ref, w_ref, mask_ref, ints_vec, floats_vec, ints_ref, floats_ref, stage, recv0, recv1, recv2, tsend, trecv, csend, crecv, edge, hrecv, mrecv,
    g_send, g_recv, t_send, t_recv, c_send, c_recv, h_send, h_recv, m_send, m_recv,
    load_sem,
):
    me = lax.axis_index("tm")
    tile = lax.axis_index("tile")
    z, y = me // 4, lax.rem(me, 4)
    peers = [lax.rem(z + dz, 4) * 4 + lax.rem(y + dy, 4) for dz, dy in OFFSETS]
    above, below = lax.rem(tile + 7, 8), lax.rem(tile + 1, 8)
    nchunk = len(CHUNKS)
    recv = (recv0, recv1, recv2)

    loads = [
        pltpu.make_async_copy(src, dst, load_sem.at[k])
        for k, (src, dst) in enumerate(((x_hbm, x_ref), (w_hbm, w_ref), (mask_hbm, mask_ref)))
    ]
    for load in loads:
        load.start()
    barrier = pltpu.get_barrier_semaphore()
    for p in peers:
        pl.semaphore_signal(barrier, inc=1, device_id={"tm": p}, device_id_type=MESH)
    for t in (above, below):
        pl.semaphore_signal(barrier, inc=1, device_id={"tile": t}, device_id_type=MESH)

    write_tables(days, me, swath_ref, ints_vec, floats_vec)
    loads += [
        pltpu.make_async_copy(ints_vec, ints_ref, load_sem.at[3]),
        pltpu.make_async_copy(floats_vec, floats_ref, load_sem.at[4]),
    ]
    for load in loads[3:]:
        load.start()
    for load in loads:
        load.wait()

    def place(k, _):
        i = ints_ref[lax.rem(k, 2), k // 2]
        for c in range(nchunk):
            stage[c, k, 0] = x_ref[i, 4 * c : 4 * c + 4]
            stage[c, k, 1] = w_ref[i, 4 * c : 4 * c + 4]
        return _

    lax.fori_loop(0, days, place, 0)
    for j in range(2):
        i = ints_ref[j, me]
        for c in range(nchunk):
            recv[c][2 * me + j, 0] = x_ref[i, 4 * c : 4 * c + 4]
            recv[c][2 * me + j, 1] = w_ref[i, 4 * c : 4 * c + 4]
    pl.semaphore_wait(barrier, len(peers) + 2)

    def remote(src, dst, send, arrive, where):
        pltpu.make_async_remote_copy(
            src_ref=src, dst_ref=dst, send_sem=send, recv_sem=arrive,
            device_id=where, device_id_type=MESH,
        ).start()

    def send_granules(c):
        for p in peers:
            remote(
                stage.at[c, pl.ds(2 * p, 2)], recv[c].at[pl.ds(2 * me, 2)],
                g_send.at[c], g_recv.at[c], {"tm": p},
            )

    def block_totals(c):
        wait_bytes(recv[c].at[pl.ds(0, 30)], g_recv.at[c])
        for g in range(4 // GROUP):
            def add(d, state):
                zeroth, first, second, level, slope = state
                a, u = floats_ref[0, d], floats_ref[1, d]
                s = ints_ref[2, d]
                v = recv[c][s, 0, GROUP * g : GROUP * (g + 1)].astype(jnp.float32)
                w = recv[c][s, 1, GROUP * g : GROUP * (g + 1)].astype(jnp.float32) * a
                wu = w * u
                p = w * v
                return (zeroth + w, first + wu, second + wu * u, level + p, slope + p * u)

            empty = jnp.zeros((GROUP, 16, 128), jnp.float32)
            state = lax.fori_loop(0, days, add, (empty,) * 5)
            for m in range(5):
                for q in range(GROUP):
                    for k in range(4):
                        tsend[c, 4 * (GROUP * g + q) + k, m] = state[m][q, 4 * k : 4 * k + 4, :]
        trecv[c, me] = tsend[c, me]
        for p in peers:
            remote(tsend.at[c, p], trecv.at[c, me], t_send.at[c], t_recv.at[c], {"tm": p})

    factor, offset = DECAY**days, days / UNIT

    def carries(c):
        wait_bytes(trecv.at[c, pl.ds(0, 15)], t_recv.at[c])
        state = [jnp.zeros((4, 128), jnp.float32)] * 5
        for b in range(16):
            zeroth, first, second, level, slope = state
            moved = (
                factor * zeroth,
                factor * (first + offset * zeroth),
                factor * (second + (2 * offset) * first + (offset * offset) * zeroth),
                factor * level,
                factor * (slope + offset * level),
            )
            for m in range(5):
                csend[c, b, m] = moved[m]
            state = [moved[m] + trecv[c, b, m] for m in range(5)]
        crecv[c, me] = csend[c, me]
        for p in peers:
            remote(csend.at[c, p], crecv.at[c, me], c_send.at[c], c_recv.at[c], {"tm": p})

    def slopes(c):
        wait_bytes(crecv.at[c, pl.ds(0, 15)], c_recv.at[c])
        for g in range(4 // GROUP):
            start = tuple(
                jnp.stack([
                    jnp.concatenate([crecv[c, 4 * (GROUP * g + q) + k, m] for k in range(4)], axis=0)
                    for q in range(GROUP)
                ])
                for m in range(5)
            )

            def advance(d, state):
                zeroth, first, second, level, slope = state
                s = ints_ref[2, d]
                a, u, ridge = (floats_ref[n, d] for n in range(3))
                v = recv[c][s, 0, GROUP * g : GROUP * (g + 1)].astype(jnp.float32)
                w = recv[c][s, 1, GROUP * g : GROUP * (g + 1)].astype(jnp.float32) * a
                wu = w * u
                p = w * v
                zeroth, first, second = zeroth + w, first + wu, second + wu * u
                level, slope = level + p, slope + p * u
                det = zeroth * (second + ridge) - first * first
                out = (first * level - zeroth * slope) / det
                for q in range(GROUP):
                    for h in range(2):
                        lanes = pl.ds(128 * (2 * (GROUP * g + q) + h), 128)
                        value = out[q, 8 * h : 8 * h + 8, :]
                        value = jnp.where(mask_ref[8 * c : 8 * c + 8, lanes] > 0, value, 0.0)
                        slope_ref[d, 8 * c : 8 * c + 8, lanes] = value
                return (zeroth, first, second, level, slope)

            lax.fori_loop(0, days, advance, start)

        def widen(d, _):
            value = lane_sum(slope_ref[d, 8 * c : 8 * c + 8])
            slope_ref[d, 8 * c : 8 * c + 8] = value
            for k in range(value.shape[1] // 128):
                if c == 0:
                    edge[0, d, k : k + 1] = value[0:1, 128 * k : 128 * k + 128]
                if c == nchunk - 1:
                    edge[1, d, k : k + 1] = value[7:8, 128 * k : 128 * k + 128]
            return _

        lax.fori_loop(0, days, widen, 0)
        if c == 0:
            remote(edge.at[0], hrecv.at[1], h_send.at[0], h_recv.at[1], {"tile": above})
        if c == nchunk - 1:
            remote(edge.at[1], hrecv.at[0], h_send.at[1], h_recv.at[0], {"tile": below})

    remote(mask_ref.at[0:8], mrecv.at[1], m_send.at[0], m_recv.at[1], {"tile": above})
    remote(mask_ref.at[16:24], mrecv.at[0], m_send.at[1], m_recv.at[0], {"tile": below})

    first, middle, last = CHUNKS
    send_granules(first)
    send_granules(middle)
    block_totals(first)
    send_granules(last)
    block_totals(middle)
    carries(first)
    block_totals(last)
    carries(middle)
    slopes(first)
    carries(last)
    slopes(middle)
    slopes(last)

    for n in range(2):
        wait_bytes(mrecv.at[n], m_recv.at[n])
        wait_bytes(hrecv.at[n], h_recv.at[n])
    for n, present in enumerate((tile > 0, tile < 7)):
        inner = jnp.where(present, 1, 0)
        halo_ref[n] = hrecv[n] * inner.astype(jnp.float32)
        mhalo_ref[n] = mrecv[n] * inner
    for c in range(nchunk):
        wait_bytes(stage.at[c, pl.ds(0, 30)], g_send.at[c])
        wait_bytes(tsend.at[c, pl.ds(0, 15)], t_send.at[c])
        wait_bytes(csend.at[c, pl.ds(0, 15)], c_send.at[c])
    for n in range(2):
        wait_bytes(edge.at[n], h_send.at[n])
        wait_bytes(mask_ref.at[0:8], m_send.at[n])


def lane_sum(field):
    width = field.shape[1]
    column = lax.broadcasted_iota(jnp.int32, field.shape, 1)
    left = jnp.where(column == 0, 0.0, pltpu.roll(field, 1, 1))
    right = jnp.where(column == width - 1, 0.0, pltpu.roll(field, width - 1, 1))
    return field + left + right


def row_sum(field, up, down):
    return (
        field
        + jnp.concatenate([up, field[:-1]], axis=0)
        + jnp.concatenate([field[1:], down], axis=0)
    )


def row_of(pieces):
    return jnp.concatenate([pieces[k : k + 1] for k in range(pieces.shape[0])], axis=1)


def smooth_kernel(per, wide_ref, halo_ref, mask_ref, mhalo_ref, out_ref, inverse, ready, sems):
    count = row_sum(
        mask_ref[...].astype(jnp.float32),
        mhalo_ref[0, 7:8].astype(jnp.float32),
        mhalo_ref[1, 0:1].astype(jnp.float32),
    )
    inverse[...] = 1.0 / jnp.maximum(lane_sum(count), 1.0)
    steps = ready.shape[0] // per

    def put(step):
        part = pl.ds(step * per, per)
        return pltpu.make_async_copy(ready.at[part], out_ref.at[part], sems.at[step])

    for step in range(steps):
        def day(n, _):
            d = step * per + n
            up = row_of(halo_ref[0, d])
            down = row_of(halo_ref[1, d])
            ready[d] = row_sum(wide_ref[d], up, down) * inverse[...]
            return _

        lax.fori_loop(0, per, day, 0)
        put(step).start()
    for step in range(steps):
        put(step).wait()


def tiled(array):
    days, rows, width = array.shape
    parts = array.reshape(days, rows // 8, 8, width // 256, 2, 128)
    return parts.transpose(0, 1, 3, 4, 2, 5).reshape(days, rows // 8 * (width // 256), 16, 128)


def on_device(ocean_heat_anomaly, observation_reliability, swath_date_number, marine_cell_flag):
    n = lax.axis_size("tm")
    days, rows, width = ocean_heat_anomaly.shape
    f32, bf16 = jnp.float32, jnp.bfloat16
    vmem = pl.BlockSpec(memory_space=pltpu.VMEM)
    hbm = pl.BlockSpec(memory_space=pltpu.HBM)
    sem = pltpu.SemaphoreType.DMA
    slope, halo, mhalo = pl.pallas_call(
        functools.partial(exchange_kernel, days),
        out_shape=(
            jax.ShapeDtypeStruct((days, rows, width), f32),
            jax.ShapeDtypeStruct((2, days, width // 128, 128), f32),
            jax.ShapeDtypeStruct((2, 8, width), jnp.int32),
        ),
        in_specs=[vmem, hbm, hbm, hbm],
        out_specs=(vmem, vmem, vmem),
        scratch_shapes=[
            pltpu.VMEM((days, rows // 8 * (width // 256), 16, 128), bf16),
            pltpu.VMEM((days, rows // 8 * (width // 256), 16, 128), bf16),
            pltpu.VMEM((rows, width), jnp.int32),
            pltpu.VMEM((8, 128), jnp.int32),
            pltpu.VMEM((8, 128), f32),
            pltpu.SMEM((8, 128), jnp.int32),
            pltpu.SMEM((8, 128), f32),
            pltpu.VMEM((3, days, 2, 4, 16, 128), bf16),
            pltpu.VMEM((days, 2, 4, 16, 128), bf16),
            pltpu.VMEM((days, 2, 4, 16, 128), bf16),
            pltpu.VMEM((days, 2, 4, 16, 128), bf16),
            pltpu.VMEM((3, n, 5, 4, 128), f32),
            pltpu.VMEM((3, n, 5, 4, 128), f32),
            pltpu.VMEM((3, n, 5, 4, 128), f32),
            pltpu.VMEM((3, n, 5, 4, 128), f32),
            pltpu.VMEM((2, days, width // 128, 128), f32),
            pltpu.VMEM((2, days, width // 128, 128), f32),
            pltpu.VMEM((2, 8, width), jnp.int32),
        ] + [sem((3,))] * 6 + [sem((2,))] * 4 + [sem((5,))],
        compiler_params=pltpu.CompilerParams(
            collective_id=0, has_side_effects=True, vmem_limit_bytes=24 << 20
        ),
    )(
        swath_date_number.reshape(4, 128),
        pltpu.with_memory_space_constraint(tiled(ocean_heat_anomaly), pltpu.HBM),
        pltpu.with_memory_space_constraint(tiled(observation_reliability), pltpu.HBM),
        pltpu.with_memory_space_constraint(marine_cell_flag, pltpu.HBM),
    )
    per = 4
    return pl.pallas_call(
        functools.partial(smooth_kernel, per),
        out_shape=jax.ShapeDtypeStruct((days, rows, width), f32),
        in_specs=[vmem] * 4,
        out_specs=pl.BlockSpec(memory_space=pl.ANY),
        scratch_shapes=[
            pltpu.VMEM((rows, width), f32),
            pltpu.VMEM((days, rows, width), f32),
            sem((days // per,)),
        ],
        compiler_params=pltpu.CompilerParams(vmem_limit_bytes=16 << 20),
    )(slope, halo, marine_cell_flag, mhalo)


def solution(mesh):
    in_specs = (P("tm", "tile", None), P("tm", "tile", None), P(), P("tile", None))
    out_specs = P("tm", "tile", None)
    return jax.shard_map(
        on_device, mesh=mesh, in_specs=in_specs, out_specs=out_specs, check_vma=False
    )
```

```python
import functools
import math

import jax
import jax.numpy as jnp
from jax import lax
from jax.experimental import pallas as pl
from jax.experimental.pallas import tpu as pltpu
from jax.sharding import PartitionSpec as P

DECAY = 0.999
UNIT = 256.0
RIDGE = 0.05
MESH = pl.DeviceIdType.MESH

OFFSETS = (
    (0, 1), (1, 0), (0, 3), (3, 0), (1, 1), (3, 3), (1, 3), (3, 1),
    (2, 0), (0, 2), (2, 1), (1, 2), (2, 3), (3, 2), (2, 2),
)
CHUNKS = (0, 2, 1)
GROUP = 2
UNROLL_ADD, UNROLL_ADVANCE, UNROLL_WIDEN, UNROLL_PLACE = 4, 4, 4, 4


def repeat(count, body, start, unroll):
    def several(k, state):
        for n in range(unroll):
            state = body(k * unroll + n, state)
        return state

    return lax.fori_loop(0, count // unroll, several, start)


def wait_bytes(ref, sem):
    pltpu.make_async_copy(ref, ref, sem).wait()


def write_tables(days, me, swath_ref, ints_vec, floats_vec):
    swath = swath_ref[...]
    row, lane = (lax.broadcasted_iota(jnp.int32, swath.shape, k) for k in range(2))
    per = 128 // days
    block, group, index = swath // days, lane // days, lax.rem(lane, days)
    source = per * row + group

    owned = jnp.sum(jnp.where(source == me, block, 0), axis=0, keepdims=True)
    number, lane16 = (lax.broadcasted_iota(jnp.int32, (16, 128), k) for k in range(2))
    index16 = lax.rem(lane16, days)
    match = (number == owned) & (lane16 // days == lax.rem(me, per))
    early = jnp.min(jnp.where(match, index16, days - 1), axis=1, keepdims=True)
    late = jnp.max(jnp.where(match, index16, 0), axis=1, keepdims=True)
    diagonal = number == lane16
    ints_vec[0:1] = jnp.sum(jnp.where(diagonal, early, 0), axis=0, keepdims=True)
    ints_vec[1:2] = jnp.sum(jnp.where(diagonal, late, 0), axis=0, keepdims=True)

    second = jnp.zeros(swath.shape, jnp.int32)
    for g in range(per):
        inside = (block == me) & (group == g)
        latest = jnp.max(jnp.where(inside, index, -1), axis=1, keepdims=True)
        second = jnp.where(inside & (index == latest), 1, second)
    slot = 2 * source + second
    day, lane32 = (lax.broadcasted_iota(jnp.int32, (days, 128), k) for k in range(2))
    hit = jnp.zeros((days, 128), jnp.int32)
    for r in range(swath.shape[0]):
        hit += jnp.where(swath[r : r + 1] == days * me + day, slot[r : r + 1], 0)
    arrived = jnp.clip(jnp.sum(hit, axis=1, keepdims=True), 0, days - 1)
    ints_vec[2:3] = jnp.sum(jnp.where(day == lane32, arrived, 0), axis=0, keepdims=True)

    lag = (days - 1 - lax.broadcasted_iota(jnp.int32, (1, 128), 1)).astype(jnp.float32)
    decay = jnp.exp(lag * math.log(DECAY))
    floats_vec[0:1] = decay
    floats_vec[1:2] = lag * (1.0 / UNIT)
    floats_vec[2:3] = RIDGE * decay


def exchange_kernel(
    days, swath_hbm, x_hbm, w_hbm, mask_hbm,
    slope_ref, halo_ref, mhalo_ref,
    swath_ref, x_ref, w_ref, mask_ref, ints_vec, floats_vec, ints_ref, floats_ref, stage, recv0, recv1, recv2, tsend, trecv, csend, crecv, edge, hrecv, mrecv,
    g_send, g_recv, t_send, t_recv, c_send, c_recv, h_send, h_recv, m_send, m_recv,
    load_sem,
):
    me = lax.axis_index("tm")
    tile = lax.axis_index("tile")
    z, y = me // 4, lax.rem(me, 4)
    peers = [lax.rem(z + dz, 4) * 4 + lax.rem(y + dy, 4) for dz, dy in OFFSETS]
    above, below = lax.rem(tile + 7, 8), lax.rem(tile + 1, 8)
    nchunk = len(CHUNKS)
    recv = (recv0, recv1, recv2)

    pairs = ((swath_hbm, swath_ref), (x_hbm, x_ref), (w_hbm, w_ref), (mask_hbm, mask_ref))
    loads = [
        pltpu.make_async_copy(src, dst, load_sem.at[k]) for k, (src, dst) in enumerate(pairs)
    ]
    for load in loads:
        load.start()
    barrier = pltpu.get_barrier_semaphore()
    for p in peers:
        pl.semaphore_signal(barrier, inc=1, device_id={"tm": p}, device_id_type=MESH)
    for t in (above, below):
        pl.semaphore_signal(barrier, inc=1, device_id={"tile": t}, device_id_type=MESH)

    loads[0].wait()
    write_tables(days, me, swath_ref, ints_vec, floats_vec)
    loads += [
        pltpu.make_async_copy(ints_vec, ints_ref, load_sem.at[4]),
        pltpu.make_async_copy(floats_vec, floats_ref, load_sem.at[5]),
    ]
    for load in loads[4:]:
        load.start()
    for load in loads[1:]:
        load.wait()

    def stage_chunk(c):
        def place(k, _):
            i = ints_ref[lax.rem(k, 2), k // 2]
            stage[c, k, 0] = x_ref[i, 4 * c : 4 * c + 4]
            stage[c, k, 1] = w_ref[i, 4 * c : 4 * c + 4]
            return _

        repeat(days, place, 0, UNROLL_PLACE)
        for j in range(2):
            i = ints_ref[j, me]
            recv[c][2 * me + j, 0] = x_ref[i, 4 * c : 4 * c + 4]
            recv[c][2 * me + j, 1] = w_ref[i, 4 * c : 4 * c + 4]

    stage_chunk(CHUNKS[0])
    pl.semaphore_wait(barrier, len(peers) + 2)

    def remote(src, dst, send, arrive, where):
        pltpu.make_async_remote_copy(
            src_ref=src, dst_ref=dst, send_sem=send, recv_sem=arrive,
            device_id=where, device_id_type=MESH,
        ).start()

    def send_granules(c):
        for p in peers:
            remote(
                stage.at[c, pl.ds(2 * p, 2)], recv[c].at[pl.ds(2 * me, 2)],
                g_send.at[c], g_recv.at[c], {"tm": p},
            )

    def block_totals(c):
        wait_bytes(recv[c].at[pl.ds(0, 30)], g_recv.at[c])
        for g in range(4 // GROUP):
            def add(d, state):
                zeroth, first, second, level, slope = state
                a, u = floats_ref[0, d], floats_ref[1, d]
                s = ints_ref[2, d]
                v = recv[c][s, 0, GROUP * g : GROUP * (g + 1)].astype(jnp.float32)
                w = recv[c][s, 1, GROUP * g : GROUP * (g + 1)].astype(jnp.float32) * a
                wu = w * u
                p = w * v
                return (zeroth + w, first + wu, second + wu * u, level + p, slope + p * u)

            empty = jnp.zeros((GROUP, 16, 128), jnp.float32)
            state = repeat(days, add, (empty,) * 5, UNROLL_ADD)
            for m in range(5):
                for q in range(GROUP):
                    for k in range(4):
                        tsend[c, 4 * (GROUP * g + q) + k, m] = state[m][q, 4 * k : 4 * k + 4, :]
        trecv[c, me] = tsend[c, me]
        for p in peers:
            remote(tsend.at[c, p], trecv.at[c, me], t_send.at[c], t_recv.at[c], {"tm": p})

    factor, offset = DECAY**days, days / UNIT

    def carries(c):
        wait_bytes(trecv.at[c, pl.ds(0, 15)], t_recv.at[c])
        state = [jnp.zeros((4, 128), jnp.float32)] * 5
        for b in range(16):
            zeroth, first, second, level, slope = state
            moved = (
                factor * zeroth,
                factor * (first + offset * zeroth),
                factor * (second + (2 * offset) * first + (offset * offset) * zeroth),
                factor * level,
                factor * (slope + offset * level),
            )
            for m in range(5):
                csend[c, b, m] = moved[m]
            state = [moved[m] + trecv[c, b, m] for m in range(5)]
        crecv[c, me] = csend[c, me]
        for p in peers:
            remote(csend.at[c, p], crecv.at[c, me], c_send.at[c], c_recv.at[c], {"tm": p})

    def slopes(c):
        wait_bytes(crecv.at[c, pl.ds(0, 15)], c_recv.at[c])
        for g in range(4 // GROUP):
            start = tuple(
                jnp.stack([
                    jnp.concatenate([crecv[c, 4 * (GROUP * g + q) + k, m] for k in range(4)], axis=0)
                    for q in range(GROUP)
                ])
                for m in range(5)
            )

            def advance(d, state):
                zeroth, first, second, level, slope = state
                s = ints_ref[2, d]
                a, u, ridge = (floats_ref[n, d] for n in range(3))
                v = recv[c][s, 0, GROUP * g : GROUP * (g + 1)].astype(jnp.float32)
                w = recv[c][s, 1, GROUP * g : GROUP * (g + 1)].astype(jnp.float32) * a
                wu = w * u
                p = w * v
                zeroth, first, second = zeroth + w, first + wu, second + wu * u
                level, slope = level + p, slope + p * u
                det = zeroth * (second + ridge) - first * first
                out = (first * level - zeroth * slope) / det
                for q in range(GROUP):
                    for h in range(2):
                        lanes = pl.ds(128 * (2 * (GROUP * g + q) + h), 128)
                        value = out[q, 8 * h : 8 * h + 8, :]
                        value = jnp.where(mask_ref[8 * c : 8 * c + 8, lanes] > 0, value, 0.0)
                        slope_ref[d, 8 * c : 8 * c + 8, lanes] = value
                return (zeroth, first, second, level, slope)

            repeat(days, advance, start, UNROLL_ADVANCE)

        def widen(d, _):
            value = lane_sum(slope_ref[d, 8 * c : 8 * c + 8])
            slope_ref[d, 8 * c : 8 * c + 8] = value
            for k in range(value.shape[1] // 128):
                if c == 0:
                    edge[0, d, k : k + 1] = value[0:1, 128 * k : 128 * k + 128]
                if c == nchunk - 1:
                    edge[1, d, k : k + 1] = value[7:8, 128 * k : 128 * k + 128]
            return _

        repeat(days, widen, 0, UNROLL_WIDEN)
        if c == 0:
            remote(edge.at[0], hrecv.at[1], h_send.at[0], h_recv.at[1], {"tile": above})
        if c == nchunk - 1:
            remote(edge.at[1], hrecv.at[0], h_send.at[1], h_recv.at[0], {"tile": below})

    remote(mask_ref.at[0:8], mrecv.at[1], m_send.at[0], m_recv.at[1], {"tile": above})
    remote(mask_ref.at[16:24], mrecv.at[0], m_send.at[1], m_recv.at[0], {"tile": below})

    first, middle, last = CHUNKS
    send_granules(first)
    stage_chunk(middle)
    send_granules(middle)
    stage_chunk(last)
    block_totals(first)
    send_granules(last)
    block_totals(middle)
    carries(first)
    block_totals(last)
    carries(middle)
    slopes(first)
    carries(last)
    slopes(middle)
    slopes(last)

    for n in range(2):
        wait_bytes(mrecv.at[n], m_recv.at[n])
        wait_bytes(hrecv.at[n], h_recv.at[n])
    for n, present in enumerate((tile > 0, tile < 7)):
        inner = jnp.where(present, 1, 0)
        halo_ref[n] = hrecv[n] * inner.astype(jnp.float32)
        mhalo_ref[n] = mrecv[n] * inner
    for c in range(nchunk):
        wait_bytes(stage.at[c, pl.ds(0, 30)], g_send.at[c])
        wait_bytes(tsend.at[c, pl.ds(0, 15)], t_send.at[c])
        wait_bytes(csend.at[c, pl.ds(0, 15)], c_send.at[c])
    for n in range(2):
        wait_bytes(edge.at[n], h_send.at[n])
        wait_bytes(mask_ref.at[0:8], m_send.at[n])


def lane_sum(field):
    width = field.shape[1]
    column = lax.broadcasted_iota(jnp.int32, field.shape, 1)
    left = jnp.where(column == 0, 0.0, pltpu.roll(field, 1, 1))
    right = jnp.where(column == width - 1, 0.0, pltpu.roll(field, width - 1, 1))
    return field + left + right


def row_sum(field, up, down):
    return (
        field
        + jnp.concatenate([up, field[:-1]], axis=0)
        + jnp.concatenate([field[1:], down], axis=0)
    )


def row_of(pieces):
    return jnp.concatenate([pieces[k : k + 1] for k in range(pieces.shape[0])], axis=1)


def smooth_kernel(per, wide_ref, halo_ref, mask_ref, mhalo_ref, out_ref, inverse, ready, sems):
    count = row_sum(
        mask_ref[...].astype(jnp.float32),
        mhalo_ref[0, 7:8].astype(jnp.float32),
        mhalo_ref[1, 0:1].astype(jnp.float32),
    )
    inverse[...] = 1.0 / jnp.maximum(lane_sum(count), 1.0)
    steps = ready.shape[0] // per

    def put(step):
        part = pl.ds(step * per, per)
        return pltpu.make_async_copy(ready.at[part], out_ref.at[part], sems.at[step])

    for step in range(steps):
        def day(n, _):
            d = step * per + n
            up = row_of(halo_ref[0, d])
            down = row_of(halo_ref[1, d])
            ready[d] = row_sum(wide_ref[d], up, down) * inverse[...]
            return _

        repeat(per, day, 0, per)
        put(step).start()
    for step in range(steps):
        put(step).wait()


def tiled(array):
    days, rows, width = array.shape
    parts = array.reshape(days, rows // 8, 8, width // 256, 2, 128)
    return parts.transpose(0, 1, 3, 4, 2, 5).reshape(days, rows // 8 * (width // 256), 16, 128)


def on_device(ocean_heat_anomaly, observation_reliability, swath_date_number, marine_cell_flag):
    n = lax.axis_size("tm")
    days, rows, width = ocean_heat_anomaly.shape
    f32, bf16 = jnp.float32, jnp.bfloat16
    vmem = pl.BlockSpec(memory_space=pltpu.VMEM)
    hbm = pl.BlockSpec(memory_space=pltpu.HBM)
    sem = pltpu.SemaphoreType.DMA
    slope, halo, mhalo = pl.pallas_call(
        functools.partial(exchange_kernel, days),
        out_shape=(
            jax.ShapeDtypeStruct((days, rows, width), f32),
            jax.ShapeDtypeStruct((2, days, width // 128, 128), f32),
            jax.ShapeDtypeStruct((2, 8, width), jnp.int32),
        ),
        in_specs=[hbm] * 4,
        out_specs=(vmem, vmem, vmem),
        scratch_shapes=[
            pltpu.VMEM((4, 128), jnp.int32),
            pltpu.VMEM((days, rows // 8 * (width // 256), 16, 128), bf16),
            pltpu.VMEM((days, rows // 8 * (width // 256), 16, 128), bf16),
            pltpu.VMEM((rows, width), jnp.int32),
            pltpu.VMEM((8, 128), jnp.int32),
            pltpu.VMEM((8, 128), f32),
            pltpu.SMEM((8, 128), jnp.int32),
            pltpu.SMEM((8, 128), f32),
            pltpu.VMEM((3, days, 2, 4, 16, 128), bf16),
            pltpu.VMEM((days, 2, 4, 16, 128), bf16),
            pltpu.VMEM((days, 2, 4, 16, 128), bf16),
            pltpu.VMEM((days, 2, 4, 16, 128), bf16),
            pltpu.VMEM((3, n, 5, 4, 128), f32),
            pltpu.VMEM((3, n, 5, 4, 128), f32),
            pltpu.VMEM((3, n, 5, 4, 128), f32),
            pltpu.VMEM((3, n, 5, 4, 128), f32),
            pltpu.VMEM((2, days, width // 128, 128), f32),
            pltpu.VMEM((2, days, width // 128, 128), f32),
            pltpu.VMEM((2, 8, width), jnp.int32),
        ] + [sem((3,))] * 6 + [sem((2,))] * 4 + [sem((6,))],
        compiler_params=pltpu.CompilerParams(
            collective_id=0, has_side_effects=True, vmem_limit_bytes=24 << 20
        ),
    )(
        pltpu.with_memory_space_constraint(swath_date_number.reshape(4, 128), pltpu.HBM),
        pltpu.with_memory_space_constraint(tiled(ocean_heat_anomaly), pltpu.HBM),
        pltpu.with_memory_space_constraint(tiled(observation_reliability), pltpu.HBM),
        pltpu.with_memory_space_constraint(marine_cell_flag, pltpu.HBM),
    )
    per = 4
    return pl.pallas_call(
        functools.partial(smooth_kernel, per),
        out_shape=jax.ShapeDtypeStruct((days, rows, width), f32),
        in_specs=[vmem] * 4,
        out_specs=pl.BlockSpec(memory_space=pl.ANY),
        scratch_shapes=[
            pltpu.VMEM((rows, width), f32),
            pltpu.VMEM((days, rows, width), f32),
            sem((days // per,)),
        ],
        compiler_params=pltpu.CompilerParams(vmem_limit_bytes=16 << 20),
    )(slope, halo, marine_cell_flag, mhalo)


def solution(mesh):
    in_specs = (P("tm", "tile", None), P("tm", "tile", None), P(), P("tile", None))
    out_specs = P("tm", "tile", None)
    return jax.shard_map(
        on_device, mesh=mesh, in_specs=in_specs, out_specs=out_specs, check_vma=False
    )
```

```python
import functools
import math

import jax
import jax.numpy as jnp
from jax import lax
from jax.experimental import pallas as pl
from jax.experimental.pallas import tpu as pltpu
from jax.sharding import PartitionSpec as P

DECAY = 0.999
UNIT = 256.0
RIDGE = 0.05
MESH = pl.DeviceIdType.MESH

OFFSETS = (
    (2, 2), (2, 1), (1, 2), (2, 3), (3, 2), (2, 0), (0, 2), (1, 1),
    (3, 3), (1, 3), (3, 1), (0, 1), (1, 0), (0, 3), (3, 0),
)
CHUNKS = (0, 2, 1)
GROUP = 2
UNROLL_ADD, UNROLL_ADVANCE, UNROLL_WIDEN, UNROLL_PLACE = 4, 4, 4, 4


def repeat(count, body, start, unroll):
    def several(k, state):
        for n in range(unroll):
            state = body(k * unroll + n, state)
        return state

    return lax.fori_loop(0, count // unroll, several, start)


def wait_bytes(ref, sem):
    pltpu.make_async_copy(ref, ref, sem).wait()


def write_tables(days, me, swath_ref, ints_vec, floats_vec):
    swath = swath_ref[...]
    row, lane = (lax.broadcasted_iota(jnp.int32, swath.shape, k) for k in range(2))
    per = 128 // days
    block, group, index = swath // days, lane // days, lax.rem(lane, days)
    source = per * row + group

    owned = jnp.sum(jnp.where(source == me, block, 0), axis=0, keepdims=True)
    number, lane16 = (lax.broadcasted_iota(jnp.int32, (16, 128), k) for k in range(2))
    index16 = lax.rem(lane16, days)
    match = (number == owned) & (lane16 // days == lax.rem(me, per))
    early = jnp.min(jnp.where(match, index16, days - 1), axis=1, keepdims=True)
    late = jnp.max(jnp.where(match, index16, 0), axis=1, keepdims=True)
    diagonal = number == lane16
    ints_vec[0:1] = jnp.sum(jnp.where(diagonal, early, 0), axis=0, keepdims=True)
    ints_vec[1:2] = jnp.sum(jnp.where(diagonal, late, 0), axis=0, keepdims=True)

    second = jnp.zeros(swath.shape, jnp.int32)
    for g in range(per):
        inside = (block == me) & (group == g)
        latest = jnp.max(jnp.where(inside, index, -1), axis=1, keepdims=True)
        second = jnp.where(inside & (index == latest), 1, second)
    slot = 2 * source + second
    day, lane32 = (lax.broadcasted_iota(jnp.int32, (days, 128), k) for k in range(2))
    hit = jnp.zeros((days, 128), jnp.int32)
    for r in range(swath.shape[0]):
        hit += jnp.where(swath[r : r + 1] == days * me + day, slot[r : r + 1], 0)
    arrived = jnp.clip(jnp.sum(hit, axis=1, keepdims=True), 0, days - 1)
    ints_vec[2:3] = jnp.sum(jnp.where(day == lane32, arrived, 0), axis=0, keepdims=True)

    lag = (days - 1 - lax.broadcasted_iota(jnp.int32, (1, 128), 1)).astype(jnp.float32)
    decay = jnp.exp(lag * math.log(DECAY))
    floats_vec[0:1] = decay
    floats_vec[1:2] = lag * (1.0 / UNIT)
    floats_vec[2:3] = RIDGE * decay


def exchange_kernel(
    days, swath_hbm, x_hbm, w_hbm, mask_hbm,
    slope_ref, halo_ref, mhalo_ref,
    swath_ref, x_ref, w_ref, mask_ref, ints_vec, floats_vec, ints_ref, floats_ref, stage, recv0, recv1, recv2, tsend, trecv, csend, crecv, edge, hrecv, mrecv,
    g_send, g_recv, t_send, t_recv, c_send, c_recv, h_send, h_recv, m_send, m_recv,
    load_sem,
):
    me = lax.axis_index("tm")
    tile = lax.axis_index("tile")
    z, y = me // 4, lax.rem(me, 4)
    peers = [lax.rem(z + dz, 4) * 4 + lax.rem(y + dy, 4) for dz, dy in OFFSETS]
    above, below = lax.rem(tile + 7, 8), lax.rem(tile + 1, 8)
    nchunk = len(CHUNKS)
    recv = (recv0, recv1, recv2)

    pairs = ((swath_hbm, swath_ref), (x_hbm, x_ref), (w_hbm, w_ref), (mask_hbm, mask_ref))
    loads = [
        pltpu.make_async_copy(src, dst, load_sem.at[k]) for k, (src, dst) in enumerate(pairs)
    ]
    for load in loads:
        load.start()
    barrier = pltpu.get_barrier_semaphore()
    for p in peers:
        pl.semaphore_signal(barrier, inc=1, device_id={"tm": p}, device_id_type=MESH)
    for t in (above, below):
        pl.semaphore_signal(barrier, inc=1, device_id={"tile": t}, device_id_type=MESH)

    loads[0].wait()
    write_tables(days, me, swath_ref, ints_vec, floats_vec)
    loads += [
        pltpu.make_async_copy(ints_vec, ints_ref, load_sem.at[4]),
        pltpu.make_async_copy(floats_vec, floats_ref, load_sem.at[5]),
    ]
    for load in loads[4:]:
        load.start()
    for load in loads[1:]:
        load.wait()

    def stage_chunk(c):
        def place(k, _):
            i = ints_ref[lax.rem(k, 2), k // 2]
            stage[c, k, 0] = x_ref[i, 4 * c : 4 * c + 4]
            stage[c, k, 1] = w_ref[i, 4 * c : 4 * c + 4]
            return _

        repeat(days, place, 0, UNROLL_PLACE)
        for j in range(2):
            i = ints_ref[j, me]
            recv[c][2 * me + j, 0] = x_ref[i, 4 * c : 4 * c + 4]
            recv[c][2 * me + j, 1] = w_ref[i, 4 * c : 4 * c + 4]

    stage_chunk(CHUNKS[0])
    pl.semaphore_wait(barrier, len(peers) + 2)

    def remote(src, dst, send, arrive, where):
        pltpu.make_async_remote_copy(
            src_ref=src, dst_ref=dst, send_sem=send, recv_sem=arrive,
            device_id=where, device_id_type=MESH,
        ).start()

    def send_granules(c):
        for p in peers:
            remote(
                stage.at[c, pl.ds(2 * p, 2)], recv[c].at[pl.ds(2 * me, 2)],
                g_send.at[c], g_recv.at[c], {"tm": p},
            )

    def block_totals(c):
        wait_bytes(recv[c].at[pl.ds(0, 30)], g_recv.at[c])
        for g in range(4 // GROUP):
            def add(d, state):
                zeroth, first, second, level, slope = state
                a, u = floats_ref[0, d], floats_ref[1, d]
                s = ints_ref[2, d]
                v = recv[c][s, 0, GROUP * g : GROUP * (g + 1)].astype(jnp.float32)
                w = recv[c][s, 1, GROUP * g : GROUP * (g + 1)].astype(jnp.float32) * a
                wu = w * u
                p = w * v
                return (zeroth + w, first + wu, second + wu * u, level + p, slope + p * u)

            empty = jnp.zeros((GROUP, 16, 128), jnp.float32)
            state = repeat(days, add, (empty,) * 5, UNROLL_ADD)
            for m in range(5):
                for q in range(GROUP):
                    for k in range(4):
                        tsend[c, 4 * (GROUP * g + q) + k, m] = state[m][q, 4 * k : 4 * k + 4, :]
        trecv[c, me] = tsend[c, me]
        for p in peers:
            remote(tsend.at[c, p], trecv.at[c, me], t_send.at[c], t_recv.at[c], {"tm": p})

    factor, offset = DECAY**days, days / UNIT

    def carries(c):
        wait_bytes(trecv.at[c, pl.ds(0, 15)], t_recv.at[c])
        state = [jnp.zeros((4, 128), jnp.float32)] * 5
        for b in range(16):
            zeroth, first, second, level, slope = state
            moved = (
                factor * zeroth,
                factor * (first + offset * zeroth),
                factor * (second + (2 * offset) * first + (offset * offset) * zeroth),
                factor * level,
                factor * (slope + offset * level),
            )
            for m in range(5):
                csend[c, b, m] = moved[m]
            state = [moved[m] + trecv[c, b, m] for m in range(5)]
        crecv[c, me] = csend[c, me]
        for p in peers:
            remote(csend.at[c, p], crecv.at[c, me], c_send.at[c], c_recv.at[c], {"tm": p})

    def slopes(c):
        wait_bytes(crecv.at[c, pl.ds(0, 15)], c_recv.at[c])
        for g in range(4 // GROUP):
            start = tuple(
                jnp.stack([
                    jnp.concatenate([crecv[c, 4 * (GROUP * g + q) + k, m] for k in range(4)], axis=0)
                    for q in range(GROUP)
                ])
                for m in range(5)
            )

            def advance(d, state):
                zeroth, first, second, level, slope = state
                s = ints_ref[2, d]
                a, u, ridge = (floats_ref[n, d] for n in range(3))
                v = recv[c][s, 0, GROUP * g : GROUP * (g + 1)].astype(jnp.float32)
                w = recv[c][s, 1, GROUP * g : GROUP * (g + 1)].astype(jnp.float32) * a
                wu = w * u
                p = w * v
                zeroth, first, second = zeroth + w, first + wu, second + wu * u
                level, slope = level + p, slope + p * u
                det = zeroth * (second + ridge) - first * first
                out = (first * level - zeroth * slope) / det
                for q in range(GROUP):
                    for h in range(2):
                        lanes = pl.ds(128 * (2 * (GROUP * g + q) + h), 128)
                        value = out[q, 8 * h : 8 * h + 8, :]
                        value = jnp.where(mask_ref[8 * c : 8 * c + 8, lanes] > 0, value, 0.0)
                        slope_ref[d, 8 * c : 8 * c + 8, lanes] = value
                return (zeroth, first, second, level, slope)

            repeat(days, advance, start, UNROLL_ADVANCE)

        def widen(d, _):
            value = lane_sum(slope_ref[d, 8 * c : 8 * c + 8])
            slope_ref[d, 8 * c : 8 * c + 8] = value
            for k in range(value.shape[1] // 128):
                if c == 0:
                    edge[0, d, k : k + 1] = value[0:1, 128 * k : 128 * k + 128]
                if c == nchunk - 1:
                    edge[1, d, k : k + 1] = value[7:8, 128 * k : 128 * k + 128]
            return _

        repeat(days, widen, 0, UNROLL_WIDEN)
        if c == 0:
            remote(edge.at[0], hrecv.at[1], h_send.at[0], h_recv.at[1], {"tile": above})
        if c == nchunk - 1:
            remote(edge.at[1], hrecv.at[0], h_send.at[1], h_recv.at[0], {"tile": below})

    remote(mask_ref.at[0:8], mrecv.at[1], m_send.at[0], m_recv.at[1], {"tile": above})
    remote(mask_ref.at[16:24], mrecv.at[0], m_send.at[1], m_recv.at[0], {"tile": below})

    first, middle, last = CHUNKS
    send_granules(first)
    stage_chunk(middle)
    send_granules(middle)
    stage_chunk(last)
    block_totals(first)
    send_granules(last)
    block_totals(middle)
    carries(first)
    block_totals(last)
    carries(middle)
    slopes(first)
    carries(last)
    slopes(middle)
    slopes(last)

    for n in range(2):
        wait_bytes(mrecv.at[n], m_recv.at[n])
        wait_bytes(hrecv.at[n], h_recv.at[n])
    for n, present in enumerate((tile > 0, tile < 7)):
        inner = jnp.where(present, 1, 0)
        halo_ref[n] = hrecv[n] * inner.astype(jnp.float32)
        mhalo_ref[n] = mrecv[n] * inner
    for c in range(nchunk):
        wait_bytes(stage.at[c, pl.ds(0, 30)], g_send.at[c])
        wait_bytes(tsend.at[c, pl.ds(0, 15)], t_send.at[c])
        wait_bytes(csend.at[c, pl.ds(0, 15)], c_send.at[c])
    for n in range(2):
        wait_bytes(edge.at[n], h_send.at[n])
        wait_bytes(mask_ref.at[0:8], m_send.at[n])


def lane_sum(field):
    width = field.shape[1]
    column = lax.broadcasted_iota(jnp.int32, field.shape, 1)
    left = jnp.where(column == 0, 0.0, pltpu.roll(field, 1, 1))
    right = jnp.where(column == width - 1, 0.0, pltpu.roll(field, width - 1, 1))
    return field + left + right


def row_sum(field, up, down):
    return (
        field
        + jnp.concatenate([up, field[:-1]], axis=0)
        + jnp.concatenate([field[1:], down], axis=0)
    )


def row_of(pieces):
    return jnp.concatenate([pieces[k : k + 1] for k in range(pieces.shape[0])], axis=1)


def smooth_kernel(per, wide_ref, halo_ref, mask_ref, mhalo_ref, out_ref, inverse, ready, sems):
    count = row_sum(
        mask_ref[...].astype(jnp.float32),
        mhalo_ref[0, 7:8].astype(jnp.float32),
        mhalo_ref[1, 0:1].astype(jnp.float32),
    )
    inverse[...] = 1.0 / jnp.maximum(lane_sum(count), 1.0)
    steps = ready.shape[0] // per

    def put(step):
        part = pl.ds(step * per, per)
        return pltpu.make_async_copy(ready.at[part], out_ref.at[part], sems.at[step])

    for step in range(steps):
        def day(n, _):
            d = step * per + n
            up = row_of(halo_ref[0, d])
            down = row_of(halo_ref[1, d])
            ready[d] = row_sum(wide_ref[d], up, down) * inverse[...]
            return _

        repeat(per, day, 0, per)
        put(step).start()
    for step in range(steps):
        put(step).wait()


def tiled(array):
    days, rows, width = array.shape
    parts = array.reshape(days, rows // 8, 8, width // 256, 2, 128)
    return parts.transpose(0, 1, 3, 4, 2, 5).reshape(days, rows // 8 * (width // 256), 16, 128)


def on_device(ocean_heat_anomaly, observation_reliability, swath_date_number, marine_cell_flag):
    n = lax.axis_size("tm")
    days, rows, width = ocean_heat_anomaly.shape
    f32, bf16 = jnp.float32, jnp.bfloat16
    vmem = pl.BlockSpec(memory_space=pltpu.VMEM)
    hbm = pl.BlockSpec(memory_space=pltpu.HBM)
    sem = pltpu.SemaphoreType.DMA
    slope, halo, mhalo = pl.pallas_call(
        functools.partial(exchange_kernel, days),
        out_shape=(
            jax.ShapeDtypeStruct((days, rows, width), f32),
            jax.ShapeDtypeStruct((2, days, width // 128, 128), f32),
            jax.ShapeDtypeStruct((2, 8, width), jnp.int32),
        ),
        in_specs=[hbm] * 4,
        out_specs=(vmem, vmem, vmem),
        scratch_shapes=[
            pltpu.VMEM((4, 128), jnp.int32),
            pltpu.VMEM((days, rows // 8 * (width // 256), 16, 128), bf16),
            pltpu.VMEM((days, rows // 8 * (width // 256), 16, 128), bf16),
            pltpu.VMEM((rows, width), jnp.int32),
            pltpu.VMEM((8, 128), jnp.int32),
            pltpu.VMEM((8, 128), f32),
            pltpu.SMEM((8, 128), jnp.int32),
            pltpu.SMEM((8, 128), f32),
            pltpu.VMEM((3, days, 2, 4, 16, 128), bf16),
            pltpu.VMEM((days, 2, 4, 16, 128), bf16),
            pltpu.VMEM((days, 2, 4, 16, 128), bf16),
            pltpu.VMEM((days, 2, 4, 16, 128), bf16),
            pltpu.VMEM((3, n, 5, 4, 128), f32),
            pltpu.VMEM((3, n, 5, 4, 128), f32),
            pltpu.VMEM((3, n, 5, 4, 128), f32),
            pltpu.VMEM((3, n, 5, 4, 128), f32),
            pltpu.VMEM((2, days, width // 128, 128), f32),
            pltpu.VMEM((2, days, width // 128, 128), f32),
            pltpu.VMEM((2, 8, width), jnp.int32),
        ] + [sem((3,))] * 6 + [sem((2,))] * 4 + [sem((6,))],
        compiler_params=pltpu.CompilerParams(
            collective_id=0, has_side_effects=True, vmem_limit_bytes=24 << 20
        ),
    )(
        pltpu.with_memory_space_constraint(swath_date_number.reshape(4, 128), pltpu.HBM),
        pltpu.with_memory_space_constraint(tiled(ocean_heat_anomaly), pltpu.HBM),
        pltpu.with_memory_space_constraint(tiled(observation_reliability), pltpu.HBM),
        pltpu.with_memory_space_constraint(marine_cell_flag, pltpu.HBM),
    )
    per = 4
    return pl.pallas_call(
        functools.partial(smooth_kernel, per),
        out_shape=jax.ShapeDtypeStruct((days, rows, width), f32),
        in_specs=[vmem] * 4,
        out_specs=pl.BlockSpec(memory_space=pl.ANY),
        scratch_shapes=[
            pltpu.VMEM((rows, width), f32),
            pltpu.VMEM((days, rows, width), f32),
            sem((days // per,)),
        ],
        compiler_params=pltpu.CompilerParams(vmem_limit_bytes=16 << 20),
    )(slope, halo, marine_cell_flag, mhalo)


def solution(mesh):
    in_specs = (P("tm", "tile", None), P("tm", "tile", None), P(), P("tile", None))
    out_specs = P("tm", "tile", None)
    return jax.shard_map(
        on_device, mesh=mesh, in_specs=in_specs, out_specs=out_specs, check_vma=False
    )
```

```python
import functools
import math

import jax
import jax.numpy as jnp
from jax import lax
from jax.experimental import pallas as pl
from jax.experimental.pallas import tpu as pltpu
from jax.sharding import PartitionSpec as P

DECAY = 0.999
UNIT = 256.0
RIDGE = 0.05
MESH = pl.DeviceIdType.MESH

OFFSETS = (
    (2, 2), (2, 1), (1, 2), (2, 3), (3, 2), (2, 0), (0, 2), (1, 1),
    (3, 3), (1, 3), (3, 1), (0, 1), (1, 0), (0, 3), (3, 0),
)
CHUNKS = (0, 2, 1)
GROUP = 2
UNROLL_ADD, UNROLL_ADVANCE, UNROLL_WIDEN, UNROLL_PLACE = 8, 8, 8, 4


def repeat(count, body, start, unroll):
    def several(k, state):
        for n in range(unroll):
            state = body(k * unroll + n, state)
        return state

    return lax.fori_loop(0, count // unroll, several, start)


def wait_bytes(ref, sem):
    pltpu.make_async_copy(ref, ref, sem).wait()


def write_tables(days, me, swath_ref, ints_vec, floats_vec):
    swath = swath_ref[...]
    row, lane = (lax.broadcasted_iota(jnp.int32, swath.shape, k) for k in range(2))
    per = 128 // days
    block, group, index = swath // days, lane // days, lax.rem(lane, days)
    source = per * row + group

    owned = jnp.sum(jnp.where(source == me, block, 0), axis=0, keepdims=True)
    number, lane16 = (lax.broadcasted_iota(jnp.int32, (16, 128), k) for k in range(2))
    index16 = lax.rem(lane16, days)
    match = (number == owned) & (lane16 // days == lax.rem(me, per))
    early = jnp.min(jnp.where(match, index16, days - 1), axis=1, keepdims=True)
    late = jnp.max(jnp.where(match, index16, 0), axis=1, keepdims=True)
    diagonal = number == lane16
    ints_vec[0:1] = jnp.sum(jnp.where(diagonal, early, 0), axis=0, keepdims=True)
    ints_vec[1:2] = jnp.sum(jnp.where(diagonal, late, 0), axis=0, keepdims=True)

    second = jnp.zeros(swath.shape, jnp.int32)
    for g in range(per):
        inside = (block == me) & (group == g)
        latest = jnp.max(jnp.where(inside, index, -1), axis=1, keepdims=True)
        second = jnp.where(inside & (index == latest), 1, second)
    slot = 2 * source + second
    day, lane32 = (lax.broadcasted_iota(jnp.int32, (days, 128), k) for k in range(2))
    hit = jnp.zeros((days, 128), jnp.int32)
    for r in range(swath.shape[0]):
        hit += jnp.where(swath[r : r + 1] == days * me + day, slot[r : r + 1], 0)
    arrived = jnp.clip(jnp.sum(hit, axis=1, keepdims=True), 0, days - 1)
    ints_vec[2:3] = jnp.sum(jnp.where(day == lane32, arrived, 0), axis=0, keepdims=True)

    lag = (days - 1 - lax.broadcasted_iota(jnp.int32, (1, 128), 1)).astype(jnp.float32)
    decay = jnp.exp(lag * math.log(DECAY))
    floats_vec[0:1] = decay
    floats_vec[1:2] = lag * (1.0 / UNIT)
    floats_vec[2:3] = RIDGE * decay


def exchange_kernel(
    days, swath_hbm, x_hbm, w_hbm, mask_hbm,
    slope_ref, halo_ref, mhalo_ref,
    swath_ref, x_ref, w_ref, mask_ref, ints_vec, floats_vec, ints_ref, floats_ref, stage, recv0, recv1, recv2, tsend, trecv, csend, crecv, edge, hrecv, mrecv,
    g_send, g_recv, t_send, t_recv, c_send, c_recv, h_send, h_recv, m_send, m_recv,
    load_sem,
):
    me = lax.axis_index("tm")
    tile = lax.axis_index("tile")
    z, y = me // 4, lax.rem(me, 4)
    peers = [lax.rem(z + dz, 4) * 4 + lax.rem(y + dy, 4) for dz, dy in OFFSETS]
    above, below = lax.rem(tile + 7, 8), lax.rem(tile + 1, 8)
    nchunk = len(CHUNKS)
    recv = (recv0, recv1, recv2)

    pairs = ((swath_hbm, swath_ref), (x_hbm, x_ref), (w_hbm, w_ref), (mask_hbm, mask_ref))
    loads = [
        pltpu.make_async_copy(src, dst, load_sem.at[k]) for k, (src, dst) in enumerate(pairs)
    ]
    for load in loads:
        load.start()
    barrier = pltpu.get_barrier_semaphore()
    for p in peers:
        pl.semaphore_signal(barrier, inc=1, device_id={"tm": p}, device_id_type=MESH)
    for t in (above, below):
        pl.semaphore_signal(barrier, inc=1, device_id={"tile": t}, device_id_type=MESH)

    loads[0].wait()
    write_tables(days, me, swath_ref, ints_vec, floats_vec)
    loads += [
        pltpu.make_async_copy(ints_vec, ints_ref, load_sem.at[4]),
        pltpu.make_async_copy(floats_vec, floats_ref, load_sem.at[5]),
    ]
    for load in loads[4:]:
        load.start()
    for load in loads[1:]:
        load.wait()

    def stage_chunk(c):
        def place(k, _):
            i = ints_ref[lax.rem(k, 2), k // 2]
            stage[c, k, 0] = x_ref[i, 4 * c : 4 * c + 4]
            stage[c, k, 1] = w_ref[i, 4 * c : 4 * c + 4]
            return _

        repeat(days, place, 0, UNROLL_PLACE)
        for j in range(2):
            i = ints_ref[j, me]
            recv[c][2 * me + j, 0] = x_ref[i, 4 * c : 4 * c + 4]
            recv[c][2 * me + j, 1] = w_ref[i, 4 * c : 4 * c + 4]

    stage_chunk(CHUNKS[0])
    pl.semaphore_wait(barrier, len(peers) + 2)

    def remote(src, dst, send, arrive, where):
        pltpu.make_async_remote_copy(
            src_ref=src, dst_ref=dst, send_sem=send, recv_sem=arrive,
            device_id=where, device_id_type=MESH,
        ).start()

    def send_granules(c):
        for p in peers:
            remote(
                stage.at[c, pl.ds(2 * p, 2)], recv[c].at[pl.ds(2 * me, 2)],
                g_send.at[c], g_recv.at[c], {"tm": p},
            )

    def block_totals(c):
        wait_bytes(recv[c].at[pl.ds(0, 30)], g_recv.at[c])
        for g in range(4 // GROUP):
            def add(d, state):
                zeroth, first, second, level, slope = state
                a, u = floats_ref[0, d], floats_ref[1, d]
                s = ints_ref[2, d]
                v = recv[c][s, 0, GROUP * g : GROUP * (g + 1)].astype(jnp.float32)
                w = recv[c][s, 1, GROUP * g : GROUP * (g + 1)].astype(jnp.float32) * a
                wu = w * u
                p = w * v
                return (zeroth + w, first + wu, second + wu * u, level + p, slope + p * u)

            empty = jnp.zeros((GROUP, 16, 128), jnp.float32)
            state = repeat(days, add, (empty,) * 5, UNROLL_ADD)
            for m in range(5):
                for q in range(GROUP):
                    for k in range(4):
                        tsend[c, 4 * (GROUP * g + q) + k, m] = state[m][q, 4 * k : 4 * k + 4, :]
        trecv[c, me] = tsend[c, me]
        for p in peers:
            remote(tsend.at[c, p], trecv.at[c, me], t_send.at[c], t_recv.at[c], {"tm": p})

    factor, offset = DECAY**days, days / UNIT

    def carries(c):
        wait_bytes(trecv.at[c, pl.ds(0, 15)], t_recv.at[c])
        state = [jnp.zeros((4, 128), jnp.float32)] * 5
        for b in range(16):
            zeroth, first, second, level, slope = state
            moved = (
                factor * zeroth,
                factor * (first + offset * zeroth),
                factor * (second + (2 * offset) * first + (offset * offset) * zeroth),
                factor * level,
                factor * (slope + offset * level),
            )
            for m in range(5):
                csend[c, b, m] = moved[m]
            state = [moved[m] + trecv[c, b, m] for m in range(5)]
        crecv[c, me] = csend[c, me]
        for p in peers:
            remote(csend.at[c, p], crecv.at[c, me], c_send.at[c], c_recv.at[c], {"tm": p})

    def slopes(c):
        wait_bytes(crecv.at[c, pl.ds(0, 15)], c_recv.at[c])
        for g in range(4 // GROUP):
            start = tuple(
                jnp.stack([
                    jnp.concatenate([crecv[c, 4 * (GROUP * g + q) + k, m] for k in range(4)], axis=0)
                    for q in range(GROUP)
                ])
                for m in range(5)
            )

            def advance(d, state):
                zeroth, first, second, level, slope = state
                s = ints_ref[2, d]
                a, u, ridge = (floats_ref[n, d] for n in range(3))
                v = recv[c][s, 0, GROUP * g : GROUP * (g + 1)].astype(jnp.float32)
                w = recv[c][s, 1, GROUP * g : GROUP * (g + 1)].astype(jnp.float32) * a
                wu = w * u
                p = w * v
                zeroth, first, second = zeroth + w, first + wu, second + wu * u
                level, slope = level + p, slope + p * u
                det = zeroth * (second + ridge) - first * first
                out = (first * level - zeroth * slope) / det
                for q in range(GROUP):
                    for h in range(2):
                        lanes = pl.ds(128 * (2 * (GROUP * g + q) + h), 128)
                        value = out[q, 8 * h : 8 * h + 8, :]
                        value = jnp.where(mask_ref[8 * c : 8 * c + 8, lanes] > 0, value, 0.0)
                        slope_ref[d, 8 * c : 8 * c + 8, lanes] = value
                return (zeroth, first, second, level, slope)

            repeat(days, advance, start, UNROLL_ADVANCE)

        def widen(d, _):
            value = lane_sum(slope_ref[d, 8 * c : 8 * c + 8])
            slope_ref[d, 8 * c : 8 * c + 8] = value
            for k in range(value.shape[1] // 128):
                if c == 0:
                    edge[0, d, k : k + 1] = value[0:1, 128 * k : 128 * k + 128]
                if c == nchunk - 1:
                    edge[1, d, k : k + 1] = value[7:8, 128 * k : 128 * k + 128]
            return _

        repeat(days, widen, 0, UNROLL_WIDEN)
        if c == 0:
            remote(edge.at[0], hrecv.at[1], h_send.at[0], h_recv.at[1], {"tile": above})
        if c == nchunk - 1:
            remote(edge.at[1], hrecv.at[0], h_send.at[1], h_recv.at[0], {"tile": below})

    remote(mask_ref.at[0:8], mrecv.at[1], m_send.at[0], m_recv.at[1], {"tile": above})
    remote(mask_ref.at[16:24], mrecv.at[0], m_send.at[1], m_recv.at[0], {"tile": below})

    first, middle, last = CHUNKS
    send_granules(first)
    stage_chunk(middle)
    send_granules(middle)
    stage_chunk(last)
    block_totals(first)
    send_granules(last)
    block_totals(middle)
    carries(first)
    block_totals(last)
    carries(middle)
    slopes(first)
    carries(last)
    slopes(middle)
    slopes(last)

    for n in range(2):
        wait_bytes(mrecv.at[n], m_recv.at[n])
        wait_bytes(hrecv.at[n], h_recv.at[n])
    for n, present in enumerate((tile > 0, tile < 7)):
        inner = jnp.where(present, 1, 0)
        halo_ref[n] = hrecv[n] * inner.astype(jnp.float32)
        mhalo_ref[n] = mrecv[n] * inner
    for c in range(nchunk):
        wait_bytes(stage.at[c, pl.ds(0, 30)], g_send.at[c])
        wait_bytes(tsend.at[c, pl.ds(0, 15)], t_send.at[c])
        wait_bytes(csend.at[c, pl.ds(0, 15)], c_send.at[c])
    for n in range(2):
        wait_bytes(edge.at[n], h_send.at[n])
        wait_bytes(mask_ref.at[0:8], m_send.at[n])


def lane_sum(field):
    width = field.shape[1]
    column = lax.broadcasted_iota(jnp.int32, field.shape, 1)
    left = jnp.where(column == 0, 0.0, pltpu.roll(field, 1, 1))
    right = jnp.where(column == width - 1, 0.0, pltpu.roll(field, width - 1, 1))
    return field + left + right


def row_sum(field, up, down):
    return (
        field
        + jnp.concatenate([up, field[:-1]], axis=0)
        + jnp.concatenate([field[1:], down], axis=0)
    )


def row_of(pieces):
    return jnp.concatenate([pieces[k : k + 1] for k in range(pieces.shape[0])], axis=1)


def smooth_kernel(per, wide_ref, halo_ref, mask_ref, mhalo_ref, out_ref, inverse, ready, sems):
    count = row_sum(
        mask_ref[...].astype(jnp.float32),
        mhalo_ref[0, 7:8].astype(jnp.float32),
        mhalo_ref[1, 0:1].astype(jnp.float32),
    )
    inverse[...] = 1.0 / jnp.maximum(lane_sum(count), 1.0)
    steps = ready.shape[0] // per

    def put(step):
        part = pl.ds(step * per, per)
        return pltpu.make_async_copy(ready.at[part], out_ref.at[part], sems.at[step])

    for step in range(steps):
        def day(n, _):
            d = step * per + n
            up = row_of(halo_ref[0, d])
            down = row_of(halo_ref[1, d])
            ready[d] = row_sum(wide_ref[d], up, down) * inverse[...]
            return _

        repeat(per, day, 0, per)
        put(step).start()
    for step in range(steps):
        put(step).wait()


def tiled(array):
    days, rows, width = array.shape
    parts = array.reshape(days, rows // 8, 8, width // 256, 2, 128)
    return parts.transpose(0, 1, 3, 4, 2, 5).reshape(days, rows // 8 * (width // 256), 16, 128)


def on_device(ocean_heat_anomaly, observation_reliability, swath_date_number, marine_cell_flag):
    n = lax.axis_size("tm")
    days, rows, width = ocean_heat_anomaly.shape
    f32, bf16 = jnp.float32, jnp.bfloat16
    vmem = pl.BlockSpec(memory_space=pltpu.VMEM)
    hbm = pl.BlockSpec(memory_space=pltpu.HBM)
    sem = pltpu.SemaphoreType.DMA
    slope, halo, mhalo = pl.pallas_call(
        functools.partial(exchange_kernel, days),
        out_shape=(
            jax.ShapeDtypeStruct((days, rows, width), f32),
            jax.ShapeDtypeStruct((2, days, width // 128, 128), f32),
            jax.ShapeDtypeStruct((2, 8, width), jnp.int32),
        ),
        in_specs=[hbm] * 4,
        out_specs=(vmem, vmem, vmem),
        scratch_shapes=[
            pltpu.VMEM((4, 128), jnp.int32),
            pltpu.VMEM((days, rows // 8 * (width // 256), 16, 128), bf16),
            pltpu.VMEM((days, rows // 8 * (width // 256), 16, 128), bf16),
            pltpu.VMEM((rows, width), jnp.int32),
            pltpu.VMEM((8, 128), jnp.int32),
            pltpu.VMEM((8, 128), f32),
            pltpu.SMEM((8, 128), jnp.int32),
            pltpu.SMEM((8, 128), f32),
            pltpu.VMEM((3, days, 2, 4, 16, 128), bf16),
            pltpu.VMEM((days, 2, 4, 16, 128), bf16),
            pltpu.VMEM((days, 2, 4, 16, 128), bf16),
            pltpu.VMEM((days, 2, 4, 16, 128), bf16),
            pltpu.VMEM((3, n, 5, 4, 128), f32),
            pltpu.VMEM((3, n, 5, 4, 128), f32),
            pltpu.VMEM((3, n, 5, 4, 128), f32),
            pltpu.VMEM((3, n, 5, 4, 128), f32),
            pltpu.VMEM((2, days, width // 128, 128), f32),
            pltpu.VMEM((2, days, width // 128, 128), f32),
            pltpu.VMEM((2, 8, width), jnp.int32),
        ] + [sem((3,))] * 6 + [sem((2,))] * 4 + [sem((6,))],
        compiler_params=pltpu.CompilerParams(
            collective_id=0, has_side_effects=True, vmem_limit_bytes=24 << 20
        ),
    )(
        pltpu.with_memory_space_constraint(swath_date_number.reshape(4, 128), pltpu.HBM),
        pltpu.with_memory_space_constraint(tiled(ocean_heat_anomaly), pltpu.HBM),
        pltpu.with_memory_space_constraint(tiled(observation_reliability), pltpu.HBM),
        pltpu.with_memory_space_constraint(marine_cell_flag, pltpu.HBM),
    )
    per = 4
    return pl.pallas_call(
        functools.partial(smooth_kernel, per),
        out_shape=jax.ShapeDtypeStruct((days, rows, width), f32),
        in_specs=[vmem] * 4,
        out_specs=pl.BlockSpec(memory_space=pl.ANY),
        scratch_shapes=[
            pltpu.VMEM((rows, width), f32),
            pltpu.VMEM((days, rows, width), f32),
            sem((days // per,)),
        ],
        compiler_params=pltpu.CompilerParams(vmem_limit_bytes=16 << 20),
    )(slope, halo, marine_cell_flag, mhalo)


def solution(mesh):
    in_specs = (P("tm", "tile", None), P("tm", "tile", None), P(), P("tile", None))
    out_specs = P("tm", "tile", None)
    return jax.shard_map(
        on_device, mesh=mesh, in_specs=in_specs, out_specs=out_specs, check_vma=False
    )
```

```python
import functools
import math

import jax
import jax.numpy as jnp
from jax import lax
from jax.experimental import pallas as pl
from jax.experimental.pallas import tpu as pltpu
from jax.sharding import PartitionSpec as P

DECAY = 0.999
UNIT = 256.0
RIDGE = 0.05
MESH = pl.DeviceIdType.MESH

OFFSETS = (
    (2, 2), (2, 1), (1, 2), (2, 3), (3, 2), (2, 0), (0, 2), (1, 1),
    (3, 3), (1, 3), (3, 1), (0, 1), (1, 0), (0, 3), (3, 0),
)
CHUNKS = (0, 2, 1)
GROUP = 2
UNROLL_ADD, UNROLL_ADVANCE, UNROLL_WIDEN, UNROLL_PLACE = 16, 16, 16, 8


def repeat(count, body, start, unroll):
    def several(k, state):
        for n in range(unroll):
            state = body(k * unroll + n, state)
        return state

    return lax.fori_loop(0, count // unroll, several, start)


def wait_bytes(ref, sem):
    pltpu.make_async_copy(ref, ref, sem).wait()


def write_tables(days, me, swath_ref, ints_vec, floats_vec):
    swath = swath_ref[...]
    row, lane = (lax.broadcasted_iota(jnp.int32, swath.shape, k) for k in range(2))
    per = 128 // days
    block, group, index = swath // days, lane // days, lax.rem(lane, days)
    source = per * row + group

    owned = jnp.sum(jnp.where(source == me, block, 0), axis=0, keepdims=True)
    number, lane16 = (lax.broadcasted_iota(jnp.int32, (16, 128), k) for k in range(2))
    index16 = lax.rem(lane16, days)
    match = (number == owned) & (lane16 // days == lax.rem(me, per))
    early = jnp.min(jnp.where(match, index16, days - 1), axis=1, keepdims=True)
    late = jnp.max(jnp.where(match, index16, 0), axis=1, keepdims=True)
    diagonal = number == lane16
    ints_vec[0:1] = jnp.sum(jnp.where(diagonal, early, 0), axis=0, keepdims=True)
    ints_vec[1:2] = jnp.sum(jnp.where(diagonal, late, 0), axis=0, keepdims=True)

    second = jnp.zeros(swath.shape, jnp.int32)
    for g in range(per):
        inside = (block == me) & (group == g)
        latest = jnp.max(jnp.where(inside, index, -1), axis=1, keepdims=True)
        second = jnp.where(inside & (index == latest), 1, second)
    slot = 2 * source + second
    day, lane32 = (lax.broadcasted_iota(jnp.int32, (days, 128), k) for k in range(2))
    hit = jnp.zeros((days, 128), jnp.int32)
    for r in range(swath.shape[0]):
        hit += jnp.where(swath[r : r + 1] == days * me + day, slot[r : r + 1], 0)
    arrived = jnp.clip(jnp.sum(hit, axis=1, keepdims=True), 0, days - 1)
    ints_vec[2:3] = jnp.sum(jnp.where(day == lane32, arrived, 0), axis=0, keepdims=True)

    lag = (days - 1 - lax.broadcasted_iota(jnp.int32, (1, 128), 1)).astype(jnp.float32)
    decay = jnp.exp(lag * math.log(DECAY))
    floats_vec[0:1] = decay
    floats_vec[1:2] = lag * (1.0 / UNIT)
    floats_vec[2:3] = RIDGE * decay


def exchange_kernel(
    days, swath_hbm, x_hbm, w_hbm, mask_hbm,
    slope_ref, halo_ref, mhalo_ref,
    swath_ref, x_ref, w_ref, mask_ref, ints_vec, floats_vec, ints_ref, floats_ref, stage, recv0, recv1, recv2, tsend, trecv, csend, crecv, edge, hrecv, mrecv,
    g_send, g_recv, t_send, t_recv, c_send, c_recv, h_send, h_recv, m_send, m_recv,
    load_sem,
):
    me = lax.axis_index("tm")
    tile = lax.axis_index("tile")
    z, y = me // 4, lax.rem(me, 4)
    peers = [lax.rem(z + dz, 4) * 4 + lax.rem(y + dy, 4) for dz, dy in OFFSETS]
    above, below = lax.rem(tile + 7, 8), lax.rem(tile + 1, 8)
    nchunk = len(CHUNKS)
    recv = (recv0, recv1, recv2)

    pairs = ((swath_hbm, swath_ref), (x_hbm, x_ref), (w_hbm, w_ref), (mask_hbm, mask_ref))
    loads = [
        pltpu.make_async_copy(src, dst, load_sem.at[k]) for k, (src, dst) in enumerate(pairs)
    ]
    for load in loads:
        load.start()
    barrier = pltpu.get_barrier_semaphore()
    for p in peers:
        pl.semaphore_signal(barrier, inc=1, device_id={"tm": p}, device_id_type=MESH)
    for t in (above, below):
        pl.semaphore_signal(barrier, inc=1, device_id={"tile": t}, device_id_type=MESH)

    loads[0].wait()
    write_tables(days, me, swath_ref, ints_vec, floats_vec)
    loads += [
        pltpu.make_async_copy(ints_vec, ints_ref, load_sem.at[4]),
        pltpu.make_async_copy(floats_vec, floats_ref, load_sem.at[5]),
    ]
    for load in loads[4:]:
        load.start()
    for load in loads[1:]:
        load.wait()

    def stage_chunk(c):
        def place(k, _):
            i = ints_ref[lax.rem(k, 2), k // 2]
            stage[c, k, 0] = x_ref[i, 4 * c : 4 * c + 4]
            stage[c, k, 1] = w_ref[i, 4 * c : 4 * c + 4]
            return _

        repeat(days, place, 0, UNROLL_PLACE)
        for j in range(2):
            i = ints_ref[j, me]
            recv[c][2 * me + j, 0] = x_ref[i, 4 * c : 4 * c + 4]
            recv[c][2 * me + j, 1] = w_ref[i, 4 * c : 4 * c + 4]

    stage_chunk(CHUNKS[0])
    pl.semaphore_wait(barrier, len(peers) + 2)

    def remote(src, dst, send, arrive, where):
        pltpu.make_async_remote_copy(
            src_ref=src, dst_ref=dst, send_sem=send, recv_sem=arrive,
            device_id=where, device_id_type=MESH,
        ).start()

    def send_granules(c):
        for p in peers:
            remote(
                stage.at[c, pl.ds(2 * p, 2)], recv[c].at[pl.ds(2 * me, 2)],
                g_send.at[c], g_recv.at[c], {"tm": p},
            )

    def block_totals(c):
        wait_bytes(recv[c].at[pl.ds(0, 30)], g_recv.at[c])
        for g in range(4 // GROUP):
            def add(d, state):
                zeroth, first, second, level, slope = state
                a, u = floats_ref[0, d], floats_ref[1, d]
                s = ints_ref[2, d]
                v = recv[c][s, 0, GROUP * g : GROUP * (g + 1)].astype(jnp.float32)
                w = recv[c][s, 1, GROUP * g : GROUP * (g + 1)].astype(jnp.float32) * a
                wu = w * u
                p = w * v
                return (zeroth + w, first + wu, second + wu * u, level + p, slope + p * u)

            empty = jnp.zeros((GROUP, 16, 128), jnp.float32)
            state = repeat(days, add, (empty,) * 5, UNROLL_ADD)
            for m in range(5):
                for q in range(GROUP):
                    for k in range(4):
                        tsend[c, 4 * (GROUP * g + q) + k, m] = state[m][q, 4 * k : 4 * k + 4, :]
        trecv[c, me] = tsend[c, me]
        for p in peers:
            remote(tsend.at[c, p], trecv.at[c, me], t_send.at[c], t_recv.at[c], {"tm": p})

    factor, offset = DECAY**days, days / UNIT

    def carries(c):
        wait_bytes(trecv.at[c, pl.ds(0, 15)], t_recv.at[c])
        state = [jnp.zeros((4, 128), jnp.float32)] * 5
        for b in range(16):
            zeroth, first, second, level, slope = state
            moved = (
                factor * zeroth,
                factor * (first + offset * zeroth),
                factor * (second + (2 * offset) * first + (offset * offset) * zeroth),
                factor * level,
                factor * (slope + offset * level),
            )
            for m in range(5):
                csend[c, b, m] = moved[m]
            state = [moved[m] + trecv[c, b, m] for m in range(5)]
        crecv[c, me] = csend[c, me]
        for p in peers:
            remote(csend.at[c, p], crecv.at[c, me], c_send.at[c], c_recv.at[c], {"tm": p})

    def slopes(c):
        wait_bytes(crecv.at[c, pl.ds(0, 15)], c_recv.at[c])
        for g in range(4 // GROUP):
            start = tuple(
                jnp.stack([
                    jnp.concatenate([crecv[c, 4 * (GROUP * g + q) + k, m] for k in range(4)], axis=0)
                    for q in range(GROUP)
                ])
                for m in range(5)
            )

            def advance(d, state):
                zeroth, first, second, level, slope = state
                s = ints_ref[2, d]
                a, u, ridge = (floats_ref[n, d] for n in range(3))
                v = recv[c][s, 0, GROUP * g : GROUP * (g + 1)].astype(jnp.float32)
                w = recv[c][s, 1, GROUP * g : GROUP * (g + 1)].astype(jnp.float32) * a
                wu = w * u
                p = w * v
                zeroth, first, second = zeroth + w, first + wu, second + wu * u
                level, slope = level + p, slope + p * u
                det = zeroth * (second + ridge) - first * first
                out = (first * level - zeroth * slope) / det
                for q in range(GROUP):
                    for h in range(2):
                        lanes = pl.ds(128 * (2 * (GROUP * g + q) + h), 128)
                        value = out[q, 8 * h : 8 * h + 8, :]
                        value = jnp.where(mask_ref[8 * c : 8 * c + 8, lanes] > 0, value, 0.0)
                        slope_ref[d, 8 * c : 8 * c + 8, lanes] = value
                return (zeroth, first, second, level, slope)

            repeat(days, advance, start, UNROLL_ADVANCE)

        def widen(d, _):
            value = lane_sum(slope_ref[d, 8 * c : 8 * c + 8])
            slope_ref[d, 8 * c : 8 * c + 8] = value
            for k in range(value.shape[1] // 128):
                if c == 0:
                    edge[0, d, k : k + 1] = value[0:1, 128 * k : 128 * k + 128]
                if c == nchunk - 1:
                    edge[1, d, k : k + 1] = value[7:8, 128 * k : 128 * k + 128]
            return _

        repeat(days, widen, 0, UNROLL_WIDEN)
        if c == 0:
            remote(edge.at[0], hrecv.at[1], h_send.at[0], h_recv.at[1], {"tile": above})
        if c == nchunk - 1:
            remote(edge.at[1], hrecv.at[0], h_send.at[1], h_recv.at[0], {"tile": below})

    remote(mask_ref.at[0:8], mrecv.at[1], m_send.at[0], m_recv.at[1], {"tile": above})
    remote(mask_ref.at[16:24], mrecv.at[0], m_send.at[1], m_recv.at[0], {"tile": below})

    first, middle, last = CHUNKS
    send_granules(first)
    stage_chunk(middle)
    send_granules(middle)
    stage_chunk(last)
    block_totals(first)
    send_granules(last)
    block_totals(middle)
    carries(first)
    block_totals(last)
    carries(middle)
    slopes(first)
    carries(last)
    slopes(middle)
    slopes(last)

    for n in range(2):
        wait_bytes(mrecv.at[n], m_recv.at[n])
        wait_bytes(hrecv.at[n], h_recv.at[n])
    for n, present in enumerate((tile > 0, tile < 7)):
        inner = jnp.where(present, 1, 0)
        halo_ref[n] = hrecv[n] * inner.astype(jnp.float32)
        mhalo_ref[n] = mrecv[n] * inner
    for c in range(nchunk):
        wait_bytes(stage.at[c, pl.ds(0, 30)], g_send.at[c])
        wait_bytes(tsend.at[c, pl.ds(0, 15)], t_send.at[c])
        wait_bytes(csend.at[c, pl.ds(0, 15)], c_send.at[c])
    for n in range(2):
        wait_bytes(edge.at[n], h_send.at[n])
        wait_bytes(mask_ref.at[0:8], m_send.at[n])


def lane_sum(field):
    width = field.shape[1]
    column = lax.broadcasted_iota(jnp.int32, field.shape, 1)
    left = jnp.where(column == 0, 0.0, pltpu.roll(field, 1, 1))
    right = jnp.where(column == width - 1, 0.0, pltpu.roll(field, width - 1, 1))
    return field + left + right


def row_sum(field, up, down):
    return (
        field
        + jnp.concatenate([up, field[:-1]], axis=0)
        + jnp.concatenate([field[1:], down], axis=0)
    )


def row_of(pieces):
    return jnp.concatenate([pieces[k : k + 1] for k in range(pieces.shape[0])], axis=1)


def smooth_kernel(per, wide_ref, halo_ref, mask_ref, mhalo_ref, out_ref, inverse, ready, sems):
    count = row_sum(
        mask_ref[...].astype(jnp.float32),
        mhalo_ref[0, 7:8].astype(jnp.float32),
        mhalo_ref[1, 0:1].astype(jnp.float32),
    )
    inverse[...] = 1.0 / jnp.maximum(lane_sum(count), 1.0)
    steps = ready.shape[0] // per

    def put(step):
        part = pl.ds(step * per, per)
        return pltpu.make_async_copy(ready.at[part], out_ref.at[part], sems.at[step])

    for step in range(steps):
        def day(n, _):
            d = step * per + n
            up = row_of(halo_ref[0, d])
            down = row_of(halo_ref[1, d])
            ready[d] = row_sum(wide_ref[d], up, down) * inverse[...]
            return _

        repeat(per, day, 0, per)
        put(step).start()
    for step in range(steps):
        put(step).wait()


def tiled(array):
    days, rows, width = array.shape
    parts = array.reshape(days, rows // 8, 8, width // 256, 2, 128)
    return parts.transpose(0, 1, 3, 4, 2, 5).reshape(days, rows // 8 * (width // 256), 16, 128)


def on_device(ocean_heat_anomaly, observation_reliability, swath_date_number, marine_cell_flag):
    n = lax.axis_size("tm")
    days, rows, width = ocean_heat_anomaly.shape
    f32, bf16 = jnp.float32, jnp.bfloat16
    vmem = pl.BlockSpec(memory_space=pltpu.VMEM)
    hbm = pl.BlockSpec(memory_space=pltpu.HBM)
    sem = pltpu.SemaphoreType.DMA
    slope, halo, mhalo = pl.pallas_call(
        functools.partial(exchange_kernel, days),
        out_shape=(
            jax.ShapeDtypeStruct((days, rows, width), f32),
            jax.ShapeDtypeStruct((2, days, width // 128, 128), f32),
            jax.ShapeDtypeStruct((2, 8, width), jnp.int32),
        ),
        in_specs=[hbm] * 4,
        out_specs=(vmem, vmem, vmem),
        scratch_shapes=[
            pltpu.VMEM((4, 128), jnp.int32),
            pltpu.VMEM((days, rows // 8 * (width // 256), 16, 128), bf16),
            pltpu.VMEM((days, rows // 8 * (width // 256), 16, 128), bf16),
            pltpu.VMEM((rows, width), jnp.int32),
            pltpu.VMEM((8, 128), jnp.int32),
            pltpu.VMEM((8, 128), f32),
            pltpu.SMEM((8, 128), jnp.int32),
            pltpu.SMEM((8, 128), f32),
            pltpu.VMEM((3, days, 2, 4, 16, 128), bf16),
            pltpu.VMEM((days, 2, 4, 16, 128), bf16),
            pltpu.VMEM((days, 2, 4, 16, 128), bf16),
            pltpu.VMEM((days, 2, 4, 16, 128), bf16),
            pltpu.VMEM((3, n, 5, 4, 128), f32),
            pltpu.VMEM((3, n, 5, 4, 128), f32),
            pltpu.VMEM((3, n, 5, 4, 128), f32),
            pltpu.VMEM((3, n, 5, 4, 128), f32),
            pltpu.VMEM((2, days, width // 128, 128), f32),
            pltpu.VMEM((2, days, width // 128, 128), f32),
            pltpu.VMEM((2, 8, width), jnp.int32),
        ] + [sem((3,))] * 6 + [sem((2,))] * 4 + [sem((6,))],
        compiler_params=pltpu.CompilerParams(
            collective_id=0, has_side_effects=True, vmem_limit_bytes=24 << 20
        ),
    )(
        pltpu.with_memory_space_constraint(swath_date_number.reshape(4, 128), pltpu.HBM),
        pltpu.with_memory_space_constraint(tiled(ocean_heat_anomaly), pltpu.HBM),
        pltpu.with_memory_space_constraint(tiled(observation_reliability), pltpu.HBM),
        pltpu.with_memory_space_constraint(marine_cell_flag, pltpu.HBM),
    )
    per = 4
    return pl.pallas_call(
        functools.partial(smooth_kernel, per),
        out_shape=jax.ShapeDtypeStruct((days, rows, width), f32),
        in_specs=[vmem] * 4,
        out_specs=pl.BlockSpec(memory_space=pl.ANY),
        scratch_shapes=[
            pltpu.VMEM((rows, width), f32),
            pltpu.VMEM((days, rows, width), f32),
            sem((days // per,)),
        ],
        compiler_params=pltpu.CompilerParams(vmem_limit_bytes=16 << 20),
    )(slope, halo, marine_cell_flag, mhalo)


def solution(mesh):
    in_specs = (P("tm", "tile", None), P("tm", "tile", None), P(), P("tile", None))
    out_specs = P("tm", "tile", None)
    return jax.shard_map(
        on_device, mesh=mesh, in_specs=in_specs, out_specs=out_specs, check_vma=False
    )
```

```python
import functools
import math

import jax
import jax.numpy as jnp
from jax import lax
from jax.experimental import pallas as pl
from jax.experimental.pallas import tpu as pltpu
from jax.sharding import PartitionSpec as P

DECAY = 0.999
UNIT = 256.0
RIDGE = 0.05
MESH = pl.DeviceIdType.MESH

OFFSETS = (
    (2, 2), (2, 1), (1, 2), (2, 3), (3, 2), (2, 0), (0, 2), (1, 1),
    (3, 3), (1, 3), (3, 1), (0, 1), (1, 0), (0, 3), (3, 0),
)
CHUNKS = (0, 2, 1)
GROUP = 2
UNROLL_ADD, UNROLL_ADVANCE, UNROLL_WIDEN, UNROLL_PLACE = 16, 16, 16, 8


def repeat(count, body, start, unroll):
    def several(k, state):
        for n in range(unroll):
            state = body(k * unroll + n, state)
        return state

    return lax.fori_loop(0, count // unroll, several, start)


def wait_bytes(ref, sem):
    pltpu.make_async_copy(ref, ref, sem).wait()


def write_tables(days, me, swath_ref, ints_vec, floats_vec):
    swath = swath_ref[...]
    row, lane = (lax.broadcasted_iota(jnp.int32, swath.shape, k) for k in range(2))
    per = 128 // days
    block, group, index = swath // days, lane // days, lax.rem(lane, days)
    source = per * row + group

    owned = jnp.sum(jnp.where(source == me, block, 0), axis=0, keepdims=True)
    number, lane16 = (lax.broadcasted_iota(jnp.int32, (16, 128), k) for k in range(2))
    index16 = lax.rem(lane16, days)
    match = (number == owned) & (lane16 // days == lax.rem(me, per))
    early = jnp.min(jnp.where(match, index16, days - 1), axis=1, keepdims=True)
    late = jnp.max(jnp.where(match, index16, 0), axis=1, keepdims=True)
    diagonal = number == lane16
    ints_vec[0:1] = jnp.sum(jnp.where(diagonal, early, 0), axis=0, keepdims=True)
    ints_vec[1:2] = jnp.sum(jnp.where(diagonal, late, 0), axis=0, keepdims=True)

    second = jnp.zeros(swath.shape, jnp.int32)
    for g in range(per):
        inside = (block == me) & (group == g)
        latest = jnp.max(jnp.where(inside, index, -1), axis=1, keepdims=True)
        second = jnp.where(inside & (index == latest), 1, second)
    slot = 2 * source + second
    day, lane32 = (lax.broadcasted_iota(jnp.int32, (days, 128), k) for k in range(2))
    hit = jnp.zeros((days, 128), jnp.int32)
    for r in range(swath.shape[0]):
        hit += jnp.where(swath[r : r + 1] == days * me + day, slot[r : r + 1], 0)
    arrived = jnp.clip(jnp.sum(hit, axis=1, keepdims=True), 0, days - 1)
    ints_vec[2:3] = jnp.sum(jnp.where(day == lane32, arrived, 0), axis=0, keepdims=True)

    lag = (days - 1 - lax.broadcasted_iota(jnp.int32, (1, 128), 1)).astype(jnp.float32)
    decay = jnp.exp(lag * math.log(DECAY))
    floats_vec[0:1] = decay
    floats_vec[1:2] = lag * (1.0 / UNIT)
    floats_vec[2:3] = RIDGE * decay


def exchange_kernel(
    days, swath_hbm, x_hbm, w_hbm, mask_hbm,
    slope_ref, halo_ref, mhalo_ref,
    swath_ref, x_ref, w_ref, mask_ref, ints_vec, floats_vec, ints_ref, floats_ref, stage, recv0, recv1, recv2, tsend, trecv, csend, crecv, edge, hrecv, mrecv,
    g_send, g_recv, t_send, t_recv, c_send, c_recv, h_send, h_recv, m_send, m_recv,
    load_sem,
):
    me = lax.axis_index("tm")
    tile = lax.axis_index("tile")
    z, y = me // 4, lax.rem(me, 4)
    peers = [lax.rem(z + dz, 4) * 4 + lax.rem(y + dy, 4) for dz, dy in OFFSETS]
    above, below = lax.rem(tile + 7, 8), lax.rem(tile + 1, 8)
    nchunk = len(CHUNKS)
    recv = (recv0, recv1, recv2)

    pairs = ((swath_hbm, swath_ref), (x_hbm, x_ref), (w_hbm, w_ref), (mask_hbm, mask_ref))
    loads = [
        pltpu.make_async_copy(src, dst, load_sem.at[k]) for k, (src, dst) in enumerate(pairs)
    ]
    for load in loads:
        load.start()
    barrier = pltpu.get_barrier_semaphore()
    for p in peers:
        pl.semaphore_signal(barrier, inc=1, device_id={"tm": p}, device_id_type=MESH)
    for t in (above, below):
        pl.semaphore_signal(barrier, inc=1, device_id={"tile": t}, device_id_type=MESH)

    loads[0].wait()
    write_tables(days, me, swath_ref, ints_vec, floats_vec)
    loads += [
        pltpu.make_async_copy(ints_vec, ints_ref, load_sem.at[4]),
        pltpu.make_async_copy(floats_vec, floats_ref, load_sem.at[5]),
    ]
    for load in loads[4:]:
        load.start()
    for load in loads[1:]:
        load.wait()

    def stage_chunk(c):
        def place(k, _):
            i = ints_ref[lax.rem(k, 2), k // 2]
            stage[c, k, 0] = x_ref[i, 4 * c : 4 * c + 4]
            stage[c, k, 1] = w_ref[i, 4 * c : 4 * c + 4]
            return _

        repeat(days, place, 0, UNROLL_PLACE)
        for j in range(2):
            i = ints_ref[j, me]
            recv[c][2 * me + j, 0] = x_ref[i, 4 * c : 4 * c + 4]
            recv[c][2 * me + j, 1] = w_ref[i, 4 * c : 4 * c + 4]

    stage_chunk(CHUNKS[0])
    pl.semaphore_wait(barrier, len(peers) + 2)

    def remote(src, dst, send, arrive, where):
        pltpu.make_async_remote_copy(
            src_ref=src, dst_ref=dst, send_sem=send, recv_sem=arrive,
            device_id=where, device_id_type=MESH,
        ).start()

    def send_granules(c, targets=peers):
        for p in targets:
            remote(
                stage.at[c, pl.ds(2 * p, 2)], recv[c].at[pl.ds(2 * me, 2)],
                g_send.at[c], g_recv.at[c], {"tm": p},
            )

    def block_totals(c):
        wait_bytes(recv[c].at[pl.ds(0, 30)], g_recv.at[c])
        for g in range(4 // GROUP):
            def add(d, state):
                zeroth, first, second, level, slope = state
                a, u = floats_ref[0, d], floats_ref[1, d]
                s = ints_ref[2, d]
                v = recv[c][s, 0, GROUP * g : GROUP * (g + 1)].astype(jnp.float32)
                w = recv[c][s, 1, GROUP * g : GROUP * (g + 1)].astype(jnp.float32) * a
                wu = w * u
                p = w * v
                return (zeroth + w, first + wu, second + wu * u, level + p, slope + p * u)

            empty = jnp.zeros((GROUP, 16, 128), jnp.float32)
            state = repeat(days, add, (empty,) * 5, UNROLL_ADD)
            for m in range(5):
                for q in range(GROUP):
                    for k in range(4):
                        tsend[c, 4 * (GROUP * g + q) + k, m] = state[m][q, 4 * k : 4 * k + 4, :]
        trecv[c, me] = tsend[c, me]
        for p in peers:
            remote(tsend.at[c, p], trecv.at[c, me], t_send.at[c], t_recv.at[c], {"tm": p})

    factor, offset = DECAY**days, days / UNIT

    def carries(c):
        wait_bytes(trecv.at[c, pl.ds(0, 15)], t_recv.at[c])
        state = [jnp.zeros((4, 128), jnp.float32)] * 5
        for b in range(16):
            zeroth, first, second, level, slope = state
            moved = (
                factor * zeroth,
                factor * (first + offset * zeroth),
                factor * (second + (2 * offset) * first + (offset * offset) * zeroth),
                factor * level,
                factor * (slope + offset * level),
            )
            for m in range(5):
                csend[c, b, m] = moved[m]
            state = [moved[m] + trecv[c, b, m] for m in range(5)]
        crecv[c, me] = csend[c, me]
        for p in peers:
            remote(csend.at[c, p], crecv.at[c, me], c_send.at[c], c_recv.at[c], {"tm": p})

    def slopes(c):
        wait_bytes(crecv.at[c, pl.ds(0, 15)], c_recv.at[c])
        for g in range(4 // GROUP):
            start = tuple(
                jnp.stack([
                    jnp.concatenate([crecv[c, 4 * (GROUP * g + q) + k, m] for k in range(4)], axis=0)
                    for q in range(GROUP)
                ])
                for m in range(5)
            )

            def advance(d, state):
                zeroth, first, second, level, slope = state
                s = ints_ref[2, d]
                a, u, ridge = (floats_ref[n, d] for n in range(3))
                v = recv[c][s, 0, GROUP * g : GROUP * (g + 1)].astype(jnp.float32)
                w = recv[c][s, 1, GROUP * g : GROUP * (g + 1)].astype(jnp.float32) * a
                wu = w * u
                p = w * v
                zeroth, first, second = zeroth + w, first + wu, second + wu * u
                level, slope = level + p, slope + p * u
                det = zeroth * (second + ridge) - first * first
                out = (first * level - zeroth * slope) / det
                for q in range(GROUP):
                    for h in range(2):
                        lanes = pl.ds(128 * (2 * (GROUP * g + q) + h), 128)
                        value = out[q, 8 * h : 8 * h + 8, :]
                        value = jnp.where(mask_ref[8 * c : 8 * c + 8, lanes] > 0, value, 0.0)
                        slope_ref[d, 8 * c : 8 * c + 8, lanes] = value
                return (zeroth, first, second, level, slope)

            repeat(days, advance, start, UNROLL_ADVANCE)

        def widen(d, _):
            value = lane_sum(slope_ref[d, 8 * c : 8 * c + 8])
            slope_ref[d, 8 * c : 8 * c + 8] = value
            for k in range(value.shape[1] // 128):
                if c == 0:
                    edge[0, d, k : k + 1] = value[0:1, 128 * k : 128 * k + 128]
                if c == nchunk - 1:
                    edge[1, d, k : k + 1] = value[7:8, 128 * k : 128 * k + 128]
            return _

        repeat(days, widen, 0, UNROLL_WIDEN)
        if c == 0:
            remote(edge.at[0], hrecv.at[1], h_send.at[0], h_recv.at[1], {"tile": above})
        if c == nchunk - 1:
            remote(edge.at[1], hrecv.at[0], h_send.at[1], h_recv.at[0], {"tile": below})

    remote(mask_ref.at[0:8], mrecv.at[1], m_send.at[0], m_recv.at[1], {"tile": above})
    remote(mask_ref.at[16:24], mrecv.at[0], m_send.at[1], m_recv.at[0], {"tile": below})

    first, middle, last = CHUNKS
    send_granules(first)
    stage_chunk(middle)
    send_granules(middle, peers[:11])
    stage_chunk(last)
    block_totals(first)
    send_granules(middle, peers[11:])
    send_granules(last)
    block_totals(middle)
    carries(first)
    block_totals(last)
    carries(middle)
    slopes(first)
    carries(last)
    slopes(middle)
    slopes(last)

    for n in range(2):
        wait_bytes(mrecv.at[n], m_recv.at[n])
        wait_bytes(hrecv.at[n], h_recv.at[n])
    for n, present in enumerate((tile > 0, tile < 7)):
        inner = jnp.where(present, 1, 0)
        halo_ref[n] = hrecv[n] * inner.astype(jnp.float32)
        mhalo_ref[n] = mrecv[n] * inner
    for c in range(nchunk):
        wait_bytes(stage.at[c, pl.ds(0, 30)], g_send.at[c])
        wait_bytes(tsend.at[c, pl.ds(0, 15)], t_send.at[c])
        wait_bytes(csend.at[c, pl.ds(0, 15)], c_send.at[c])
    for n in range(2):
        wait_bytes(edge.at[n], h_send.at[n])
        wait_bytes(mask_ref.at[0:8], m_send.at[n])


def lane_sum(field):
    width = field.shape[1]
    column = lax.broadcasted_iota(jnp.int32, field.shape, 1)
    left = jnp.where(column == 0, 0.0, pltpu.roll(field, 1, 1))
    right = jnp.where(column == width - 1, 0.0, pltpu.roll(field, width - 1, 1))
    return field + left + right


def row_sum(field, up, down):
    return (
        field
        + jnp.concatenate([up, field[:-1]], axis=0)
        + jnp.concatenate([field[1:], down], axis=0)
    )


def row_of(pieces):
    return jnp.concatenate([pieces[k : k + 1] for k in range(pieces.shape[0])], axis=1)


def smooth_kernel(per, wide_ref, halo_ref, mask_ref, mhalo_ref, out_ref, inverse, ready, sems):
    count = row_sum(
        mask_ref[...].astype(jnp.float32),
        mhalo_ref[0, 7:8].astype(jnp.float32),
        mhalo_ref[1, 0:1].astype(jnp.float32),
    )
    inverse[...] = 1.0 / jnp.maximum(lane_sum(count), 1.0)
    steps = ready.shape[0] // per

    def put(step):
        part = pl.ds(step * per, per)
        return pltpu.make_async_copy(ready.at[part], out_ref.at[part], sems.at[step])

    for step in range(steps):
        def day(n, _):
            d = step * per + n
            up = row_of(halo_ref[0, d])
            down = row_of(halo_ref[1, d])
            ready[d] = row_sum(wide_ref[d], up, down) * inverse[...]
            return _

        repeat(per, day, 0, per)
        put(step).start()
    for step in range(steps):
        put(step).wait()


def tiled(array):
    days, rows, width = array.shape
    parts = array.reshape(days, rows // 8, 8, width // 256, 2, 128)
    return parts.transpose(0, 1, 3, 4, 2, 5).reshape(days, rows // 8 * (width // 256), 16, 128)


def on_device(ocean_heat_anomaly, observation_reliability, swath_date_number, marine_cell_flag):
    n = lax.axis_size("tm")
    days, rows, width = ocean_heat_anomaly.shape
    f32, bf16 = jnp.float32, jnp.bfloat16
    vmem = pl.BlockSpec(memory_space=pltpu.VMEM)
    hbm = pl.BlockSpec(memory_space=pltpu.HBM)
    sem = pltpu.SemaphoreType.DMA
    slope, halo, mhalo = pl.pallas_call(
        functools.partial(exchange_kernel, days),
        out_shape=(
            jax.ShapeDtypeStruct((days, rows, width), f32),
            jax.ShapeDtypeStruct((2, days, width // 128, 128), f32),
            jax.ShapeDtypeStruct((2, 8, width), jnp.int32),
        ),
        in_specs=[hbm] * 4,
        out_specs=(vmem, vmem, vmem),
        scratch_shapes=[
            pltpu.VMEM((4, 128), jnp.int32),
            pltpu.VMEM((days, rows // 8 * (width // 256), 16, 128), bf16),
            pltpu.VMEM((days, rows // 8 * (width // 256), 16, 128), bf16),
            pltpu.VMEM((rows, width), jnp.int32),
            pltpu.VMEM((8, 128), jnp.int32),
            pltpu.VMEM((8, 128), f32),
            pltpu.SMEM((8, 128), jnp.int32),
            pltpu.SMEM((8, 128), f32),
            pltpu.VMEM((3, days, 2, 4, 16, 128), bf16),
            pltpu.VMEM((days, 2, 4, 16, 128), bf16),
            pltpu.VMEM((days, 2, 4, 16, 128), bf16),
            pltpu.VMEM((days, 2, 4, 16, 128), bf16),
            pltpu.VMEM((3, n, 5, 4, 128), f32),
            pltpu.VMEM((3, n, 5, 4, 128), f32),
            pltpu.VMEM((3, n, 5, 4, 128), f32),
            pltpu.VMEM((3, n, 5, 4, 128), f32),
            pltpu.VMEM((2, days, width // 128, 128), f32),
            pltpu.VMEM((2, days, width // 128, 128), f32),
            pltpu.VMEM((2, 8, width), jnp.int32),
        ] + [sem((3,))] * 6 + [sem((2,))] * 4 + [sem((6,))],
        compiler_params=pltpu.CompilerParams(
            collective_id=0, has_side_effects=True, vmem_limit_bytes=24 << 20
        ),
    )(
        pltpu.with_memory_space_constraint(swath_date_number.reshape(4, 128), pltpu.HBM),
        pltpu.with_memory_space_constraint(tiled(ocean_heat_anomaly), pltpu.HBM),
        pltpu.with_memory_space_constraint(tiled(observation_reliability), pltpu.HBM),
        pltpu.with_memory_space_constraint(marine_cell_flag, pltpu.HBM),
    )
    per = 4
    return pl.pallas_call(
        functools.partial(smooth_kernel, per),
        out_shape=jax.ShapeDtypeStruct((days, rows, width), f32),
        in_specs=[vmem] * 4,
        out_specs=pl.BlockSpec(memory_space=pl.ANY),
        scratch_shapes=[
            pltpu.VMEM((rows, width), f32),
            pltpu.VMEM((days, rows, width), f32),
            sem((days // per,)),
        ],
        compiler_params=pltpu.CompilerParams(vmem_limit_bytes=16 << 20),
    )(slope, halo, marine_cell_flag, mhalo)


def solution(mesh):
    in_specs = (P("tm", "tile", None), P("tm", "tile", None), P(), P("tile", None))
    out_specs = P("tm", "tile", None)
    return jax.shard_map(
        on_device, mesh=mesh, in_specs=in_specs, out_specs=out_specs, check_vma=False
    )
```
